32 devices in a mesh: band: 4 (over x, core), pw: 8 (over z, y).
Axes of the slice: x: 2, y: 2, z: 4, core: 2. Of those that a mesh axis runs over, the one named last changes fastest.
Arguments:
- wave_coeffs: float32 [32768, 512], P('pw', 'band'), may hold values from -6 to 6
- miller: int32 [3, 32768], P(None, 'pw'), may hold values from -32 to 31, as said below
- atom_types: int32 [32], replicated, may hold values from 0 to 3
- positions: float32 [3, 32], replicated, may hold values from 0 to 1
- sphere_radii: float32 [4], replicated, may hold values from 3.5 to 5
- h_blocks: float32 [4, 64, 64], replicated, may hold values from -3 to 3
- potential: float32 [64, 64, 64], P('pw'), may hold values from -2 to 2
Outputs:
- h_applied: float32 [32768, 512], P('pw', 'band')
- subspace: float32 [512, 512], P('pw', 'band')
The draws below stay inside these ranges and needn't reach their ends.
Inputs may be any that keep to these rules, and one draw needn't show every extreme that they name: `miller`: the plane waves are distinct grid points after wrapping mod 64. The plane waves of the k-th of 8 equal contiguous blocks have wrapped z index in k * 8 to (k + 1) * 8 - 1.
All inputs are finite; a program needn't handle non-finite values.
Results may differ from the reference program's by a relative error of at most 0.0003.
Values sent between devices are 32-bit elements; how exact they have to be, the bound alone decides.
No kernel may reach another device: no remote copies, remote signals or barrier semaphores. Data moves between devices by JAX's collectives and lax.ppermute only.
A program may use at most 128 MiB of HBM per device.

```python
import math
import jax
import jax.numpy as jnp
import numpy as np
from jax import lax

NPW = 32768
BANDS = 512
GRID = 64
LMAX = 7
NF = 64
NTYPES = 4
ATOMS = 32
N_PW = 8


def draw_miller(key, part):
    planes_each = GRID // N_PW
    per_shard = NPW // N_PW

    def shard(shard_index):
        chosen = jax.random.permutation(jax.random.fold_in(key, shard_index + 11), planes_each * GRID * GRID)[:per_shard]
        z_plane = chosen // (GRID * GRID) + shard_index * planes_each
        x_col = chosen // GRID % GRID
        y_row = chosen % GRID
        return jnp.stack([x_col, y_row, z_plane])
    whole = jax.vmap(shard)(jnp.arange(N_PW, dtype=jnp.int32))
    whole = jnp.transpose(whole, (1, 0, 2)).reshape(3, NPW)
    return ((whole + GRID // 2) % GRID - GRID // 2).astype(jnp.int32)


def plant(array, own_key, least, largest):
    longest = array.shape.index(max(array.shape))
    spots = []
    for shift in (0, 1):
        where = [jax.random.randint(jax.random.fold_in(own_key, axis), (), 0, length) for axis, length in enumerate(array.shape)]
        where[longest] = (where[longest] + shift) % array.shape[longest]
        spots.append(tuple(where))
    return array.at[spots[0]].set(least).at[spots[1]].set(largest)


def steps_of(own_key, extent, split, least, largest):
    def one(dim, shards_of):
        draws = jax.random.uniform(jax.random.fold_in(jax.random.fold_in(own_key, 6), dim), (shards_of,), jnp.float32, least / len(split), largest / len(split))
        return jnp.repeat(jnp.exp(draws), extent[dim] // shards_of).reshape((-1,) + (1,) * (len(extent) - dim - 1))

    gain = one(*split[0])
    for cut in split[1:]:
        gain = gain * one(*cut)
    return gain


def gaussian(key, dims, spread, bound, pieces=(), kind=jnp.bfloat16):
    loudness = steps_of(key, dims, pieces, -0.22, 0.18) if pieces else 1.0
    values = jax.random.normal(key, dims, jnp.float32) * spread * loudness
    return jnp.minimum(jnp.maximum(values, -bound), bound).astype(kind)


def setup_inputs(seed: int = 0) -> dict:
    streams_of = jax.random.split(jax.random.key(seed), 8)
    wave_coeffs = gaussian(streams_of[0], (NPW, BANDS), 1.0, 6.0, ((0, 8), (1, 4)), jnp.float32)
    miller = draw_miller(jax.random.fold_in(streams_of[7], 71), 0)
    atom_types = plant(jax.random.randint(streams_of[2], (ATOMS,), 0, NTYPES), jax.random.fold_in(streams_of[2], 1), 0, NTYPES - 1).astype(jnp.int32)
    positions = jnp.clip(jax.random.uniform(streams_of[3], (3, ATOMS), jnp.float32, 0.0, 1.0), 0.0, 1.0)
    sphere_radii = jnp.clip(jnp.exp(jax.random.uniform(streams_of[4], (NTYPES,), jnp.float32, math.log(3.5), math.log(5.0))), 3.5, 5.0)
    h_blocks = gaussian(streams_of[5], (NTYPES, NF, NF), 0.5, 3.0, (), jnp.float32)
    potential = jnp.clip(jax.random.uniform(streams_of[6], (GRID, GRID, GRID), jnp.float32, -2.0, 2.0) * steps_of(streams_of[6], (GRID, GRID, GRID), ((0, 8),), -0.4, 0.0), -2.0, 2.0)
    return {"wave_coeffs": wave_coeffs, "miller": miller, "atom_types": atom_types, "positions": positions, "sphere_radii": sphere_radii, "h_blocks": h_blocks, "potential": potential}


PRECISE = lax.Precision.HIGHEST

def double_factorial(value):
    result = 1
    while value > 1:
        result = result * value
        value = value - 2
    return float(result)

def bessel_table(argument, count):
    safe = jnp.maximum(argument, 1.0)
    upward = [jnp.sin(safe) / safe, jnp.sin(safe) / (safe * safe) - jnp.cos(safe) / safe]
    for degree in range(1, count - 1):
        upward.append((2 * degree + 1) / safe * upward[degree] - upward[degree - 1])
    half_square = -0.5 * argument * argument
    power = jnp.ones_like(argument)
    columns = []
    for degree in range(count):
        term = jnp.ones_like(argument)
        total = jnp.ones_like(argument)
        for index in range(1, 17):
            term = term * half_square / float(index * (2 * degree + 2 * index + 1))
            total = total + term
        series = power * total / double_factorial(2 * degree + 1)
        power = power * argument
        columns.append(jnp.where(argument > degree + 1, upward[degree], series))
    return jnp.stack(columns, axis=-1)

def harmonic_table(unit, count):
    along_x, along_y, along_z = (unit[0], unit[1], unit[2])
    ones = jnp.ones_like(along_z)
    cosines = [ones]
    sines = [jnp.zeros_like(along_z)]
    for azimuth in range(1, count):
        cosines.append(along_x * cosines[-1] - along_y * sines[-1])
        sines.append(along_x * sines[-2 + 1] + along_y * cosines[-2])
    legendre = {}
    for azimuth in range(count):
        legendre[azimuth, azimuth] = double_factorial(2 * azimuth - 1) * ones
        if azimuth + 1 < count:
            legendre[azimuth + 1, azimuth] = (2 * azimuth + 1) * along_z * legendre[azimuth, azimuth]
        for degree in range(azimuth + 2, count):
            legendre[degree, azimuth] = ((2 * degree - 1) * along_z * legendre[degree - 1, azimuth] - (degree + azimuth - 1) * legendre[degree - 2, azimuth]) / float(degree - azimuth)
    columns = []
    for degree in range(count):
        for signed in range(-degree, degree + 1):
            azimuth = abs(signed)
            weight = math.sqrt((2 * degree + 1) * math.factorial(degree - azimuth) / (4.0 * math.pi * math.factorial(degree + azimuth)))
            if azimuth > 0:
                weight = weight * math.sqrt(2.0)
            circle = cosines[azimuth] if signed >= 0 else sines[azimuth]
            columns.append(weight * legendre[degree, azimuth] * circle)
    return jnp.stack(columns, axis=-1)

def cas_matrix(grid_size):
    across = jnp.arange(grid_size, dtype=jnp.int32)
    phase = across[:, None] * across[None, :] % grid_size
    angle = 2.0 * math.pi / grid_size * phase.astype(jnp.float32)
    return (jnp.cos(angle) + jnp.sin(angle)) / math.sqrt(grid_size)

def transform3(table, field):
    field = jnp.einsum('ai,ijkb->ajkb', table, field, precision=PRECISE)
    field = jnp.einsum('aj,ijkb->iakb', table, field, precision=PRECISE)
    return jnp.einsum('ak,ijkb->ijab', table, field, precision=PRECISE)

def atom_matching(miller_float, radial_rows, angular, centre):
    angle = 2.0 * math.pi * jnp.dot(miller_float.T, centre, precision=PRECISE)
    wave = jnp.cos(angle) + jnp.sin(angle)
    return wave[:, None] * radial_rows * angular * (4.0 * math.pi * NPW ** (-0.5))

def reference(wave_coeffs, miller, atom_types, positions, sphere_radii, h_blocks, potential):
    miller_float = miller.astype(jnp.float32)
    squares = lax.optimization_barrier(jnp.sum(miller_float * miller_float, axis=0))
    miller_norm = jnp.sqrt(squares)
    kinetic = squares / 1536.0
    wrapped = jnp.mod(miller, GRID).astype(jnp.int32)
    table = cas_matrix(GRID)
    degree_count = LMAX + 1
    degree_of = np.repeat(np.arange(degree_count), 2 * np.arange(degree_count) + 1)
    unit = miller_float / jnp.maximum(miller_norm, 1.0)
    angular = harmonic_table(unit, degree_count)
    argument = sphere_radii[None, :] * miller_norm[:, None] * (2.0 / GRID)
    radial_all = bessel_table(argument, degree_count)

    def interstitial_block(block):
        grid_field = jnp.zeros((GRID, GRID, GRID, block.shape[1]), jnp.float32)
        grid_field = grid_field.at[wrapped[0], wrapped[1], wrapped[2]].set(block)
        real_field = transform3(table, grid_field)
        back_field = transform3(table, real_field * potential[..., None])
        return back_field[wrapped[0], wrapped[1], wrapped[2]]
    band_blocks = wave_coeffs.reshape(NPW, BANDS // 32, 32).transpose(1, 0, 2)
    inter = lax.map(interstitial_block, band_blocks).transpose(1, 0, 2).reshape(NPW, BANDS)
    chosen = h_blocks[atom_types]

    def radial_for(kind):
        return jnp.take(radial_all, kind, axis=1)[:, degree_of]

    def forward(carry, inputs):
        centre, kind, block_h = inputs
        tile = atom_matching(miller_float, radial_for(kind), angular, centre)
        sphere = jnp.dot(tile.T, wave_coeffs, precision=PRECISE)
        return (carry, jnp.dot(block_h, sphere, precision=PRECISE))
    _, applied = lax.scan(forward, jnp.zeros((), jnp.float32), (positions.T, atom_types, chosen))

    def backward(total, inputs):
        centre, kind, values = inputs
        tile = atom_matching(miller_float, radial_for(kind), angular, centre)
        return (total + jnp.dot(tile, values, precision=PRECISE), None)
    muffin, _ = lax.scan(backward, jnp.zeros((NPW, BANDS), jnp.float32), (positions.T, atom_types, applied))
    h_applied = kinetic[:, None] * wave_coeffs + inter + muffin
    subspace = jnp.dot(wave_coeffs.T, h_applied, precision=PRECISE) * NPW ** (-0.5)
    return (h_applied, subspace)
```

```python
import functools
import math

import jax
import jax.numpy as jnp
import numpy as np
from jax import lax
from jax.experimental import pallas as pl
from jax.experimental.pallas import tpu as pltpu
from jax.sharding import PartitionSpec as P

NPW = 32768


PRECISE = lax.Precision.HIGHEST


def double_factorial(value):
    result = 1
    while value > 1:
        result = result * value
        value = value - 2
    return float(result)


def bessel_table(argument, count):
    safe = jnp.maximum(argument, 1.0)
    upward = [jnp.sin(safe) / safe, jnp.sin(safe) / (safe * safe) - jnp.cos(safe) / safe]
    for degree in range(1, count - 1):
        upward.append((2 * degree + 1) / safe * upward[degree] - upward[degree - 1])
    half_square = -0.5 * argument * argument
    power = jnp.ones_like(argument)
    columns = []
    for degree in range(count):
        term = jnp.ones_like(argument)
        total = jnp.ones_like(argument)
        for index in range(1, 17):
            term = term * half_square / float(index * (2 * degree + 2 * index + 1))
            total = total + term
        series = power * total / double_factorial(2 * degree + 1)
        power = power * argument
        columns.append(jnp.where(argument > degree + 1, upward[degree], series))
    return columns


def harmonic_table(unit, count):
    along_x, along_y, along_z = (unit[0], unit[1], unit[2])
    ones = jnp.ones_like(along_z)
    cosines = [ones]
    sines = [jnp.zeros_like(along_z)]
    for azimuth in range(1, count):
        cosines.append(along_x * cosines[-1] - along_y * sines[-1])
        sines.append(along_x * sines[-2 + 1] + along_y * cosines[-2])
    legendre = {}
    for azimuth in range(count):
        legendre[azimuth, azimuth] = double_factorial(2 * azimuth - 1) * ones
        if azimuth + 1 < count:
            legendre[azimuth + 1, azimuth] = (
                (2 * azimuth + 1) * along_z * legendre[azimuth, azimuth]
            )
        for degree in range(azimuth + 2, count):
            legendre[degree, azimuth] = (
                (2 * degree - 1) * along_z * legendre[degree - 1, azimuth]
                - (degree + azimuth - 1) * legendre[degree - 2, azimuth]
            ) / float(degree - azimuth)
    columns = []
    for degree in range(count):
        for signed in range(-degree, degree + 1):
            azimuth = abs(signed)
            weight = math.sqrt(
                (2 * degree + 1)
                * math.factorial(degree - azimuth)
                / (4.0 * math.pi * math.factorial(degree + azimuth))
            )
            if azimuth > 0:
                weight = weight * math.sqrt(2.0)
            circle = cosines[azimuth] if signed >= 0 else sines[azimuth]
            columns.append(weight * legendre[degree, azimuth] * circle)
    return columns


def cas_matrix(grid_size):
    across = jnp.arange(grid_size, dtype=jnp.int32)
    phase = across[:, None] * across[None, :] % grid_size
    angle = 2.0 * math.pi / grid_size * phase.astype(jnp.float32)
    return (jnp.cos(angle) + jnp.sin(angle)) / math.sqrt(grid_size)


def split_bf16(value):
    high = value.astype(jnp.bfloat16)
    low = (value - high.astype(jnp.float32)).astype(jnp.bfloat16)
    return high, low


def dot32(left, right):
    return jnp.dot(left, right, preferred_element_type=jnp.float32)


def params(*semantics):
    return pltpu.CompilerParams(
        dimension_semantics=semantics or None, vmem_limit_bytes=56 * 1024 * 1024
    )


def fill_matching(types_ref, table_ref, phase_ref, high_ref, low_ref):
    atoms = phase_ref.shape[0]
    funcs = table_ref.shape[1]

    def one(atom, carry):
        tile = table_ref[types_ref[atom]] * phase_ref[pl.ds(atom, 1), :]
        high, low = split_bf16(tile)
        start = pl.multiple_of(atom * funcs, funcs)
        high_ref[pl.ds(start, funcs), :] = high
        low_ref[pl.ds(start, funcs), :] = low
        return carry

    lax.fori_loop(0, atoms, one, 0, unroll=4)


def fill_tables(miller_ref, places_ref, radii_ref, table_ref, phase_ref, angular_ref, spacing):
    kinds, funcs, _ = table_ref.shape
    degree_count = math.isqrt(funcs)
    miller = miller_ref[...].astype(jnp.float32)
    along = [miller[axis : axis + 1, :] for axis in range(3)]
    norm = jnp.sqrt(along[0] * along[0] + along[1] * along[1] + along[2] * along[2])
    scale = jnp.maximum(norm, 1.0)
    for index, column in enumerate(harmonic_table([part / scale for part in along], degree_count)):
        angular_ref[index : index + 1, :] = column
    argument = radii_ref[...] * norm * spacing
    weight = 4.0 * math.pi * NPW ** (-0.5)
    for degree, column in enumerate(bessel_table(argument, degree_count)):
        first, last = degree * degree, (degree + 1) * (degree + 1)
        rows = angular_ref[first:last, :]
        for kind in range(kinds):
            table_ref[kind, first:last, :] = rows * (column[kind : kind + 1, :] * weight)
    places = places_ref[...]
    turns = sum(places[:, axis : axis + 1] * along[axis] for axis in range(3))
    angle = 2.0 * math.pi * (turns - jnp.round(turns))
    phase_ref[...] = jnp.cos(angle) + jnp.sin(angle)


def sphere_kernel(
    types_ref,
    miller_ref,
    places_ref,
    radii_ref,
    wave_ref,
    out_ref,
    table_ref,
    phase_ref,
    angular_ref,
    high_ref,
    low_ref,
    *,
    spacing,
):
    bands = wave_ref.shape[1]

    @pl.when(pl.program_id(0) == 0)
    def _():
        out_ref[...] = jnp.zeros_like(out_ref)

    fill_tables(miller_ref, places_ref, radii_ref, table_ref, phase_ref, angular_ref, spacing)
    fill_matching(types_ref, table_ref, phase_ref, high_ref, low_ref)
    wave_high, wave_low = split_bf16(wave_ref[...])
    both = jnp.concatenate([wave_high, wave_low], axis=1)
    rows = out_ref.shape[0]
    step = math.gcd(rows, 512)
    for first in range(0, rows, step):
        main = dot32(high_ref[first : first + step, :], both)
        rest = dot32(low_ref[first : first + step, :], wave_high)
        out_ref[first : first + step, :] += main[:, :bands] + main[:, bands:] + rest


def sphere_call(types, miller, positions, radii, wave, kinds, funcs, spacing):
    waves, bands = wave.shape
    atoms = positions.shape[1]
    block = math.gcd(waves, 512)
    rows = atoms * funcs
    return pl.pallas_call(
        functools.partial(sphere_kernel, spacing=spacing),
        grid=(waves // block,),
        in_specs=[
            pl.BlockSpec(memory_space=pltpu.SMEM),
            pl.BlockSpec((3, block), lambda i: (0, i)),
            pl.BlockSpec((atoms, 3), lambda i: (0, 0)),
            pl.BlockSpec((kinds, 1), lambda i: (0, 0)),
            pl.BlockSpec((block, bands), lambda i: (i, 0)),
        ],
        out_specs=[
            pl.BlockSpec((rows, bands), lambda i: (0, 0)),
            pl.BlockSpec((kinds, funcs, block), lambda i: (0, 0, i)),
            pl.BlockSpec((atoms, block), lambda i: (0, i)),
        ],
        out_shape=[
            jax.ShapeDtypeStruct((rows, bands), jnp.float32),
            jax.ShapeDtypeStruct((kinds, funcs, waves), jnp.float32),
            jax.ShapeDtypeStruct((atoms, waves), jnp.float32),
        ],
        scratch_shapes=[
            pltpu.VMEM((funcs, block), jnp.float32),
            pltpu.VMEM((rows, block), jnp.bfloat16),
            pltpu.VMEM((rows, block), jnp.bfloat16),
        ],
        compiler_params=params("arbitrary"),
        cost_estimate=pl.CostEstimate(
            flops=6 * waves * rows * bands, bytes_accessed=8 * waves * bands, transcendentals=0
        ),
        name="sphere",
    )(types, miller, positions.T, radii[:, None], wave)


def muffin_kernel(types_ref, table_ref, phase_ref, sphere_ref, out_ref, high_ref, low_ref):
    bands = out_ref.shape[0]
    fill_matching(types_ref, table_ref, phase_ref, high_ref, low_ref)
    high, low = split_bf16(sphere_ref[...])
    main = dot32(jnp.concatenate([high, low], axis=0), high_ref[...])
    rest = dot32(high, low_ref[...])
    out_ref[...] = main[:bands, :] + main[bands:, :] + rest


def muffin_call(types, table, phase, sphere):
    kinds, funcs, waves = table.shape
    atoms = phase.shape[0]
    bands, rows = sphere.shape
    block = math.gcd(waves, 512)
    return pl.pallas_call(
        muffin_kernel,
        grid=(waves // block,),
        in_specs=[
            pl.BlockSpec(memory_space=pltpu.SMEM),
            pl.BlockSpec((kinds, funcs, block), lambda i: (0, 0, i)),
            pl.BlockSpec((atoms, block), lambda i: (0, i)),
            pl.BlockSpec((bands, rows), lambda i: (0, 0)),
        ],
        out_specs=pl.BlockSpec((bands, block), lambda i: (0, i)),
        out_shape=jax.ShapeDtypeStruct((bands, waves), jnp.float32),
        scratch_shapes=[
            pltpu.VMEM((rows, block), jnp.bfloat16),
            pltpu.VMEM((rows, block), jnp.bfloat16),
        ],
        compiler_params=params("arbitrary"),
        cost_estimate=pl.CostEstimate(
            flops=6 * waves * rows * bands, bytes_accessed=8 * waves * bands, transcendentals=0
        ),
        name="muffin",
    )(types, table, phase, sphere)


def sort_kernel(rank_ref, key_ref, wave_ref, send_ref, sorted_ref, rows_ref):
    waves, bands = wave_ref.shape
    parts, _, pairs, lanes = send_ref.shape
    half = lanes // 2

    def place(index, carry):
        target = rank_ref[index]
        rows_ref[pl.ds(target, 1), :] = wave_ref[pl.ds(index, 1), :]
        sorted_ref[target] = key_ref[index]
        return carry

    lax.fori_loop(0, waves, place, 0, unroll=8)

    def turn(tile, carry):
        start = pl.multiple_of(tile * lanes, lanes)
        turned = rows_ref[pl.ds(start, lanes), :].T
        for part in range(parts):
            first = part * 2 * pairs
            top = turned[first : first + pairs, :]
            low = turned[first + pairs : first + 2 * pairs, :]
            send_ref[part, 2 * tile] = jnp.concatenate([top[:, :half], low[:, :half]], axis=1)
            send_ref[part, 2 * tile + 1] = jnp.concatenate([top[:, half:], low[:, half:]], axis=1)
        return carry

    lax.fori_loop(0, waves // lanes, turn, 0)


def sort_call(rank, key, wave, parts, half):
    waves, bands = wave.shape
    pairs = bands // parts // 2
    return pl.pallas_call(
        sort_kernel,
        in_specs=[
            pl.BlockSpec(memory_space=pltpu.SMEM),
            pl.BlockSpec(memory_space=pltpu.SMEM),
            pl.BlockSpec(memory_space=pltpu.VMEM),
        ],
        out_specs=[
            pl.BlockSpec(memory_space=pltpu.VMEM),
            pl.BlockSpec(memory_space=pltpu.SMEM),
        ],
        out_shape=[
            jax.ShapeDtypeStruct((parts, waves // half, pairs, 2 * half), jnp.float32),
            jax.ShapeDtypeStruct((waves,), jnp.int32),
        ],
        scratch_shapes=[pltpu.VMEM((waves, bands), jnp.float32)],
        compiler_params=params(),
        name="sort",
    )(rank, key, wave)


def unsort_kernel(rank_ref, back_ref, wave_ref, kinetic_ref, out_ref, rows_ref):
    waves, bands = wave_ref.shape
    parts, _, pairs, lanes = back_ref.shape
    half = lanes // 2

    def turn(tile, carry):
        start = pl.multiple_of(tile * lanes, lanes)
        pieces = []
        for part in range(parts):
            even = back_ref[part, 2 * tile]
            odd = back_ref[part, 2 * tile + 1]
            pieces.append(jnp.concatenate([even[:, :half], odd[:, :half]], axis=1))
            pieces.append(jnp.concatenate([even[:, half:], odd[:, half:]], axis=1))
        rows_ref[pl.ds(start, lanes), :] = jnp.concatenate(pieces, axis=0).T
        return carry

    lax.fori_loop(0, waves // lanes, turn, 0)

    def place(index, carry):
        out_ref[pl.ds(index, 1), :] = rows_ref[pl.ds(rank_ref[index], 1), :]
        return carry

    lax.fori_loop(0, waves, place, 0, unroll=8)
    out_ref[...] += kinetic_ref[...] * wave_ref[...]


def unsort_call(rank, back, wave, kinetic):
    waves, bands = wave.shape
    vmem = pl.BlockSpec(memory_space=pltpu.VMEM)
    return pl.pallas_call(
        unsort_kernel,
        in_specs=[pl.BlockSpec(memory_space=pltpu.SMEM), vmem, vmem, vmem],
        out_specs=vmem,
        out_shape=jax.ShapeDtypeStruct((waves, bands), jnp.float32),
        scratch_shapes=[pltpu.VMEM((waves, bands), jnp.float32)],
        compiler_params=params(),
        name="unsort",
    )(rank, back, wave, kinetic[:, None])


def lane_gather(values, index):
    return jnp.take_along_axis(values, index, axis=1, mode="promise_in_bounds")


def grid_kernel(
    starts_ref,
    first_ref,
    last_ref,
    code_ref,
    slot_row_ref,
    slot_y_ref,
    potential_ref,
    left_ref,
    right_ref,
    compact_ref,
    out_ref,
    grid_ref,
    *,
    size,
    pitch,
    band_pitch,
):
    blocks, pairs, lanes = compact_ref.shape
    half = lanes // 2
    rows = size * size
    upper = lax.broadcasted_iota(jnp.int32, (pairs, lanes), 1) // half * half
    shift = int(math.log2(half))

    def expand_one(row):
        start = starts_ref[row]
        block = jnp.minimum(start >> shift, blocks - 1)
        following = jnp.minimum(block + 1, blocks - 1)
        code = jnp.broadcast_to(code_ref[pl.ds(row, 1), :], (pairs, lanes))
        place = code + (start & (half - 1))
        index = (place & (half - 1)) | upper
        here = lane_gather(compact_ref[block], index)
        there = lane_gather(compact_ref[following], index)
        value = jnp.where(place < half, here, there)
        value = jnp.where(code >= 0, value, 0.0)
        target = (row // size) * pitch + row % size
        grid_ref[pl.ds(target, pairs, stride=band_pitch), :] = value

    def expand(group, carry):
        for step in range(8):
            expand_one(group * 8 + step)
        return carry

    lax.fori_loop(0, rows // 8, expand, 0)

    left = left_ref[...]
    right = right_ref[...]

    def apply_left(value):
        high, low = split_bf16(value)
        both = dot32(left, jnp.concatenate([high, low], axis=0))
        return both[:size, :] + both[size:, :]

    def apply_right(value):
        high, low = split_bf16(value)
        both = dot32(jnp.concatenate([high, low], axis=1), right)
        return both[:, :lanes] + both[:, lanes:]

    many = 8

    def planes(turn, carry):
        pair = turn // (size // many)
        base = pair * band_pitch + (turn % (size // many)) * many * pitch
        starts = [pl.multiple_of(base + index * pitch, 8) for index in range(many)]
        field = jnp.concatenate([grid_ref[pl.ds(s, size), :] for s in starts], axis=1)
        field = apply_left(field)
        field = jnp.concatenate(
            [field[:, index * lanes : (index + 1) * lanes] for index in range(many)], axis=0
        )
        field = apply_right(field)
        for index, s in enumerate(starts):
            grid_ref[pl.ds(s, size), :] = field[index * size : (index + 1) * size, :]
        return carry

    def columns(turn, carry):
        pair = turn // (size // many)
        along = (turn % (size // many)) * many
        base = pair * band_pitch + along
        field = jnp.concatenate(
            [grid_ref[pl.ds(base + index, size, stride=pitch), :] for index in range(many)], axis=1
        )
        field = apply_left(field)
        weight = jnp.concatenate(
            [
                potential_ref[pl.ds(pl.multiple_of((along + index) * size, size), size), :]
                for index in range(many)
            ],
            axis=1,
        )
        field = apply_left(field * weight)
        for index in range(many):
            grid_ref[pl.ds(base + index, size, stride=pitch), :] = field[
                :, index * lanes : (index + 1) * lanes
            ]
        return carry

    turns = pairs * (size // many)
    lax.fori_loop(0, turns, planes, 0)
    lax.fori_loop(0, turns, columns, 0)
    lax.fori_loop(0, turns, planes, 0)

    def collect(block, carry):
        wanted = jnp.broadcast_to(slot_row_ref[pl.ds(block, 1), :], (pairs, lanes))
        index = jnp.broadcast_to(slot_y_ref[pl.ds(block, 1), :], (pairs, lanes))
        first = first_ref[block]
        trips = (last_ref[block] - first) // many + 1

        def some(trip, value):
            for step in range(many):
                row = jnp.minimum(first + trip * many + step, rows - 1)
                source = (row // size) * pitch + row % size
                here = lane_gather(grid_ref[pl.ds(source, pairs, stride=band_pitch), :], index)
                value = jnp.where(wanted == row, here, value)
            return value

        out_ref[block] = lax.fori_loop(0, trips, some, jnp.zeros((pairs, lanes), jnp.float32))
        return carry

    lax.fori_loop(0, blocks, collect, 0)


def grid_call(starts, first, last, code, slot_row, slot_y, potential, left, right, compact, size):
    blocks, pairs, lanes = compact.shape
    pitch = size + 8
    band_pitch = size * pitch + 8
    smem = pl.BlockSpec(memory_space=pltpu.SMEM)
    vmem = pl.BlockSpec(memory_space=pltpu.VMEM)
    points = 2 * pairs * size**3
    return pl.pallas_call(
        functools.partial(grid_kernel, size=size, pitch=pitch, band_pitch=band_pitch),
        in_specs=[smem] * 3 + [vmem] * 7,
        out_specs=vmem,
        out_shape=jax.ShapeDtypeStruct(compact.shape, jnp.float32),
        scratch_shapes=[pltpu.VMEM((pairs * band_pitch, lanes), jnp.float32)],
        compiler_params=params(),
        cost_estimate=pl.CostEstimate(
            flops=36 * size * points, bytes_accessed=4 * points, transcendentals=0
        ),
        name="grid",
    )(starts, first, last, code, slot_row, slot_y, potential, left, right, compact)


def finish_kernel(muffin_ref, rest_ref, all_ref, out_ref, sub_ref):
    bands = out_ref.shape[1]

    @pl.when(pl.program_id(0) == 0)
    def _():
        sub_ref[...] = jnp.zeros_like(sub_ref)

    applied = muffin_ref[...] + rest_ref[...].T
    out_ref[...] = applied.T
    high, low = split_bf16(applied)
    all_high, all_low = split_bf16(all_ref[...])
    main = dot32(jnp.concatenate([high, low], axis=0), all_high)
    sub_ref[...] += main[:bands, :] + main[bands:, :] + dot32(high, all_low)


def finish_call(muffin, rest, columns):
    waves, bands = rest.shape
    total = columns.shape[1]
    block = math.gcd(waves, 512)
    return pl.pallas_call(
        finish_kernel,
        grid=(waves // block,),
        in_specs=[
            pl.BlockSpec((bands, block), lambda i: (0, i)),
            pl.BlockSpec((block, bands), lambda i: (i, 0)),
            pl.BlockSpec((block, total), lambda i: (i, 0)),
        ],
        out_specs=[
            pl.BlockSpec((block, bands), lambda i: (i, 0)),
            pl.BlockSpec((bands, total), lambda i: (0, 0)),
        ],
        out_shape=[
            jax.ShapeDtypeStruct((waves, bands), jnp.float32),
            jax.ShapeDtypeStruct((bands, total), jnp.float32),
        ],
        compiler_params=params("arbitrary"),
        name="finish",
    )(muffin, rest, columns)


def exchange(array):
    return lax.all_to_all(array, "pw", split_axis=0, concat_axis=0, tiled=True)


def round_high(value):
    return lax.reduce_precision(value, 8, 7)


def interstitial_tables(size):
    table = cas_matrix(size)
    high = round_high(table)
    low = round_high(table - high)
    zero = jnp.zeros_like(table)
    left = jnp.concatenate(
        [jnp.concatenate([high, high], axis=1), jnp.concatenate([low, zero], axis=1)], axis=0
    )

    def twice(block):
        return jnp.concatenate(
            [jnp.concatenate([block, zero], axis=1), jnp.concatenate([zero, block], axis=1)], axis=0
        )

    right = jnp.concatenate(
        [
            jnp.concatenate([twice(high), twice(low)], axis=1),
            jnp.concatenate([twice(high), jnp.zeros((2 * size, 2 * size))], axis=1),
        ],
        axis=0,
    )
    return left.astype(jnp.bfloat16), right.astype(jnp.bfloat16)


def per_device(wave_coeffs, miller, atom_types, positions, sphere_radii, h_blocks, potential):
    pw_count = lax.axis_size("pw")
    pw_index = lax.axis_index("pw")
    local_waves, local_bands = wave_coeffs.shape
    size = potential.shape[1]
    kinds, funcs_each = h_blocks.shape[:2]
    atom_total = atom_types.shape[0]
    factor = NPW ** (-0.5)
    miller_float = miller.astype(jnp.float32)
    kinetic = jnp.sum(miller_float * miller_float, axis=0) / 1536.0
    planes_each = size // pw_count
    lines = planes_each * size

    wrapped = jnp.mod(miller, size)
    line = (wrapped[2] - pw_index * planes_each) * size + wrapped[0]
    key = line * size + wrapped[1]
    rank = jnp.sum((key[:, None] < key[None, :]).astype(jnp.int32), axis=0)
    starts = jnp.sum(
        (line[:, None] < jnp.arange(lines, dtype=jnp.int32)[None, :]).astype(jnp.int32), axis=0
    )
    line_onehot = (line[None, :] == jnp.arange(lines, dtype=jnp.int32)[:, None]).astype(
        jnp.bfloat16
    )
    across = jnp.arange(size, dtype=jnp.int32)
    y_onehot = (wrapped[1][:, None] == across[None, :]).astype(jnp.bfloat16)
    filled = jnp.dot(line_onehot, y_onehot, preferred_element_type=jnp.float32)
    before = (across[:, None] < across[None, :]).astype(jnp.bfloat16)
    ahead = jnp.dot(filled.astype(jnp.bfloat16), before, preferred_element_type=jnp.float32)
    code = jnp.where(filled > 0.5, ahead, -1024.0)

    send, sorted_key = sort_call(rank, key, wave_coeffs, pw_count, size)
    turned = jnp.transpose(potential, (0, 2, 1))
    pieces = [
        turned.reshape(-1),
        code.reshape(-1),
        starts.astype(jnp.float32),
        sorted_key.astype(jnp.float32),
    ]
    cuts = np.cumsum([piece.shape[0] for piece in pieces])
    known = lax.all_gather(jnp.concatenate(pieces), "pw", axis=0, tiled=False)
    compact = exchange(send)

    spheres, matching_table, phase = sphere_call(
        atom_types, miller, positions, sphere_radii, wave_coeffs, kinds, funcs_each, 2.0 / size
    )
    atoms_each = atom_total // pw_count
    parts = exchange(spheres.reshape(pw_count, atoms_each * funcs_each, local_bands))
    mine = jnp.sum(parts, axis=0).reshape(atoms_each, funcs_each, local_bands)
    own_types = lax.dynamic_slice_in_dim(atom_types, pw_index * atoms_each, atoms_each, 0)
    own_onehot = (own_types[:, None] == jnp.arange(kinds, dtype=jnp.int32)[None, :]).astype(
        jnp.float32
    )
    chosen = jnp.einsum("at,tfk->afk", own_onehot, h_blocks, precision=PRECISE)
    applied = jnp.einsum("akb,afk->baf", mine, chosen, precision=PRECISE).reshape(
        1, local_bands, atoms_each * funcs_each
    )
    applied = exchange(jnp.broadcast_to(applied, (pw_count,) + applied.shape[1:]))
    applied = jnp.transpose(applied, (1, 0, 2)).reshape(local_bands, atom_total * funcs_each)

    wave_again, known = lax.optimization_barrier((wave_coeffs, known))
    columns = lax.all_gather(wave_again, "band", axis=1, tiled=True)

    field = known[:, : cuts[0]].reshape(size * size, size)
    field = jnp.concatenate([field, field], axis=1)
    codes = known[:, cuts[0] : cuts[1]].reshape(size * size, size).astype(jnp.int32)
    codes = jnp.concatenate([codes, codes], axis=1)
    offsets = jnp.arange(pw_count, dtype=jnp.int32)[:, None]
    all_starts = known[:, cuts[1] : cuts[2]].astype(jnp.int32) + offsets * local_waves
    all_keys = known[:, cuts[2] : cuts[3]].astype(jnp.int32)
    all_keys = (all_keys + offsets * (lines * size)).reshape(-1, size)
    slot_row = all_keys // size
    slot_y = all_keys % size
    left, right = interstitial_tables(size)
    back = grid_call(
        all_starts.reshape(-1),
        slot_row[:, 0],
        slot_row[:, -1],
        codes,
        jnp.concatenate([slot_row, slot_row], axis=1),
        jnp.concatenate([slot_y, slot_y + size], axis=1),
        field,
        left,
        right,
        compact.reshape(-1, *compact.shape[2:]),
        size,
    )
    back = exchange(back.reshape(compact.shape))
    muffin = muffin_call(atom_types, matching_table, phase, applied)
    rest = unsort_call(rank, back, wave_coeffs, kinetic)
    h_applied, partial = finish_call(muffin, rest, columns)
    partial = jnp.transpose(partial) * factor
    rows_each = partial.shape[0] // pw_count
    gathered = exchange(partial.reshape(pw_count, rows_each, local_bands))
    return (h_applied, jnp.sum(gathered, axis=0))


def solution(mesh):
    in_specs = (P("pw", "band"), P(None, "pw"), P(), P(), P(), P(), P("pw", None, None))
    out_specs = (P("pw", "band"), P("pw", "band"))
    return jax.shard_map(
        per_device, mesh=mesh, in_specs=in_specs, out_specs=out_specs, check_vma=False
    )
```

```python
import functools
import math

import jax
import jax.numpy as jnp
import numpy as np
from jax import lax
from jax.experimental import pallas as pl
from jax.experimental.pallas import tpu as pltpu
from jax.sharding import PartitionSpec as P

NPW = 32768


PRECISE = lax.Precision.HIGHEST


def double_factorial(value):
    result = 1
    while value > 1:
        result = result * value
        value = value - 2
    return float(result)


def bessel_table(argument, count):
    safe = jnp.maximum(argument, 1.0)
    upward = [jnp.sin(safe) / safe, jnp.sin(safe) / (safe * safe) - jnp.cos(safe) / safe]
    for degree in range(1, count - 1):
        upward.append((2 * degree + 1) / safe * upward[degree] - upward[degree - 1])
    half_square = -0.5 * argument * argument
    power = jnp.ones_like(argument)
    columns = []
    for degree in range(count):
        term = jnp.ones_like(argument)
        total = jnp.ones_like(argument)
        for index in range(1, 17):
            term = term * half_square / float(index * (2 * degree + 2 * index + 1))
            total = total + term
        series = power * total / double_factorial(2 * degree + 1)
        power = power * argument
        columns.append(jnp.where(argument > degree + 1, upward[degree], series))
    return columns


def harmonic_table(unit, count):
    along_x, along_y, along_z = (unit[0], unit[1], unit[2])
    ones = jnp.ones_like(along_z)
    cosines = [ones]
    sines = [jnp.zeros_like(along_z)]
    for azimuth in range(1, count):
        cosines.append(along_x * cosines[-1] - along_y * sines[-1])
        sines.append(along_x * sines[-2 + 1] + along_y * cosines[-2])
    legendre = {}
    for azimuth in range(count):
        legendre[azimuth, azimuth] = double_factorial(2 * azimuth - 1) * ones
        if azimuth + 1 < count:
            legendre[azimuth + 1, azimuth] = (
                (2 * azimuth + 1) * along_z * legendre[azimuth, azimuth]
            )
        for degree in range(azimuth + 2, count):
            legendre[degree, azimuth] = (
                (2 * degree - 1) * along_z * legendre[degree - 1, azimuth]
                - (degree + azimuth - 1) * legendre[degree - 2, azimuth]
            ) / float(degree - azimuth)
    columns = []
    for degree in range(count):
        for signed in range(-degree, degree + 1):
            azimuth = abs(signed)
            weight = math.sqrt(
                (2 * degree + 1)
                * math.factorial(degree - azimuth)
                / (4.0 * math.pi * math.factorial(degree + azimuth))
            )
            if azimuth > 0:
                weight = weight * math.sqrt(2.0)
            circle = cosines[azimuth] if signed >= 0 else sines[azimuth]
            columns.append(weight * legendre[degree, azimuth] * circle)
    return columns


def cas_matrix(grid_size):
    across = jnp.arange(grid_size, dtype=jnp.int32)
    phase = across[:, None] * across[None, :] % grid_size
    angle = 2.0 * math.pi / grid_size * phase.astype(jnp.float32)
    return (jnp.cos(angle) + jnp.sin(angle)) / math.sqrt(grid_size)


def split_bf16(value):
    high = value.astype(jnp.bfloat16)
    low = (value - high.astype(jnp.float32)).astype(jnp.bfloat16)
    return high, low


def dot32(left, right):
    return jnp.dot(left, right, preferred_element_type=jnp.float32)


def params(*semantics):
    return pltpu.CompilerParams(
        dimension_semantics=semantics or None, vmem_limit_bytes=56 * 1024 * 1024
    )


def fill_matching(types_ref, table_ref, phase_ref, high_ref, low_ref):
    atoms = phase_ref.shape[0]
    funcs = table_ref.shape[1]

    def one(atom, carry):
        tile = table_ref[types_ref[atom]] * phase_ref[pl.ds(atom, 1), :]
        high, low = split_bf16(tile)
        start = pl.multiple_of(atom * funcs, funcs)
        high_ref[pl.ds(start, funcs), :] = high
        low_ref[pl.ds(start, funcs), :] = low
        return carry

    lax.fori_loop(0, atoms, one, 0, unroll=4)


def fill_tables(miller_ref, places_ref, radii_ref, table_ref, phase_ref, angular_ref, spacing):
    kinds, funcs, _ = table_ref.shape
    degree_count = math.isqrt(funcs)
    miller = miller_ref[...].astype(jnp.float32)
    along = [miller[axis : axis + 1, :] for axis in range(3)]
    norm = jnp.sqrt(along[0] * along[0] + along[1] * along[1] + along[2] * along[2])
    scale = jnp.maximum(norm, 1.0)
    for index, column in enumerate(harmonic_table([part / scale for part in along], degree_count)):
        angular_ref[index : index + 1, :] = column
    argument = radii_ref[...] * norm * spacing
    weight = 4.0 * math.pi * NPW ** (-0.5)
    for degree, column in enumerate(bessel_table(argument, degree_count)):
        first, last = degree * degree, (degree + 1) * (degree + 1)
        rows = angular_ref[first:last, :]
        for kind in range(kinds):
            table_ref[kind, first:last, :] = rows * (column[kind : kind + 1, :] * weight)
    places = places_ref[...]
    turns = sum(places[:, axis : axis + 1] * along[axis] for axis in range(3))
    angle = 2.0 * math.pi * (turns - jnp.round(turns))
    phase_ref[...] = jnp.cos(angle) + jnp.sin(angle)


def sphere_kernel(
    types_ref,
    miller_ref,
    places_ref,
    radii_ref,
    wave_ref,
    out_ref,
    table_ref,
    phase_ref,
    angular_ref,
    high_ref,
    low_ref,
    *,
    spacing,
):
    bands = wave_ref.shape[1]

    @pl.when(pl.program_id(0) == 0)
    def _():
        out_ref[...] = jnp.zeros_like(out_ref)

    fill_tables(miller_ref, places_ref, radii_ref, table_ref, phase_ref, angular_ref, spacing)
    fill_matching(types_ref, table_ref, phase_ref, high_ref, low_ref)
    wave_high, wave_low = split_bf16(wave_ref[...])
    both = jnp.concatenate([wave_high, wave_low], axis=1)
    rows = out_ref.shape[0]
    step = math.gcd(rows, 512)
    for first in range(0, rows, step):
        main = dot32(high_ref[first : first + step, :], both)
        rest = dot32(low_ref[first : first + step, :], wave_high)
        out_ref[first : first + step, :] += main[:, :bands] + main[:, bands:] + rest


def sphere_call(types, miller, positions, radii, wave, kinds, funcs, spacing):
    waves, bands = wave.shape
    atoms = positions.shape[1]
    block = math.gcd(waves, 512)
    rows = atoms * funcs
    return pl.pallas_call(
        functools.partial(sphere_kernel, spacing=spacing),
        grid=(waves // block,),
        in_specs=[
            pl.BlockSpec(memory_space=pltpu.SMEM),
            pl.BlockSpec((3, block), lambda i: (0, i)),
            pl.BlockSpec((atoms, 3), lambda i: (0, 0)),
            pl.BlockSpec((kinds, 1), lambda i: (0, 0)),
            pl.BlockSpec((block, bands), lambda i: (i, 0)),
        ],
        out_specs=[
            pl.BlockSpec((rows, bands), lambda i: (0, 0)),
            pl.BlockSpec((kinds, funcs, block), lambda i: (0, 0, i)),
            pl.BlockSpec((atoms, block), lambda i: (0, i)),
        ],
        out_shape=[
            jax.ShapeDtypeStruct((rows, bands), jnp.float32),
            jax.ShapeDtypeStruct((kinds, funcs, waves), jnp.float32),
            jax.ShapeDtypeStruct((atoms, waves), jnp.float32),
        ],
        scratch_shapes=[
            pltpu.VMEM((funcs, block), jnp.float32),
            pltpu.VMEM((rows, block), jnp.bfloat16),
            pltpu.VMEM((rows, block), jnp.bfloat16),
        ],
        compiler_params=params("arbitrary"),
        cost_estimate=pl.CostEstimate(
            flops=6 * waves * rows * bands, bytes_accessed=8 * waves * bands, transcendentals=0
        ),
        name="sphere",
    )(types, miller, positions.T, radii[:, None], wave)


def muffin_kernel(
    types_ref,
    table_ref,
    phase_ref,
    sphere_ref,
    kinetic_ref,
    wave_ref,
    out_ref,
    high_ref,
    low_ref,
):
    bands = out_ref.shape[0]
    fill_matching(types_ref, table_ref, phase_ref, high_ref, low_ref)
    high, low = split_bf16(sphere_ref[...])
    main = dot32(jnp.concatenate([high, low], axis=0), high_ref[...])
    rest = dot32(high, low_ref[...])
    kinetic = kinetic_ref[...] * wave_ref[...].T
    out_ref[...] = main[:bands, :] + main[bands:, :] + rest + kinetic


def muffin_call(types, table, phase, sphere, kinetic, wave):
    kinds, funcs, waves = table.shape
    atoms = phase.shape[0]
    bands, rows = sphere.shape
    block = math.gcd(waves, 512)
    return pl.pallas_call(
        muffin_kernel,
        grid=(waves // block,),
        in_specs=[
            pl.BlockSpec(memory_space=pltpu.SMEM),
            pl.BlockSpec((kinds, funcs, block), lambda i: (0, 0, i)),
            pl.BlockSpec((atoms, block), lambda i: (0, i)),
            pl.BlockSpec((bands, rows), lambda i: (0, 0)),
            pl.BlockSpec((1, block), lambda i: (0, i)),
            pl.BlockSpec((block, bands), lambda i: (i, 0)),
        ],
        out_specs=pl.BlockSpec((bands, block), lambda i: (0, i)),
        out_shape=jax.ShapeDtypeStruct((bands, waves), jnp.float32),
        scratch_shapes=[
            pltpu.VMEM((rows, block), jnp.bfloat16),
            pltpu.VMEM((rows, block), jnp.bfloat16),
        ],
        compiler_params=params("arbitrary"),
        cost_estimate=pl.CostEstimate(
            flops=6 * waves * rows * bands, bytes_accessed=8 * waves * bands, transcendentals=0
        ),
        name="muffin",
    )(types, table, phase, sphere, kinetic[None, :], wave)


def sort_kernel(rank_ref, key_ref, wave_ref, send_ref, sorted_ref, rows_ref):
    waves, _ = wave_ref.shape
    parts, _, pairs, lanes = send_ref.shape
    half = lanes // 2

    def place(index, carry):
        target = rank_ref[index]
        rows_ref[pl.ds(target, 1), :] = wave_ref[pl.ds(index, 1), :]
        sorted_ref[target] = key_ref[index]
        return carry

    lax.fori_loop(0, waves, place, 0, unroll=32)

    def turn(tile, carry):
        start = pl.multiple_of(tile * lanes, lanes)
        turned = rows_ref[pl.ds(start, lanes), :].T
        for part in range(parts):
            first = part * 2 * pairs
            top = turned[first : first + pairs, :]
            low = turned[first + pairs : first + 2 * pairs, :]
            send_ref[part, 2 * tile] = jnp.concatenate([top[:, :half], low[:, :half]], axis=1)
            send_ref[part, 2 * tile + 1] = jnp.concatenate([top[:, half:], low[:, half:]], axis=1)
        return carry

    lax.fori_loop(0, waves // lanes, turn, 0)


def sort_call(rank, key, wave, parts, half):
    waves, bands = wave.shape
    pairs = bands // parts // 2
    return pl.pallas_call(
        sort_kernel,
        in_specs=[
            pl.BlockSpec(memory_space=pltpu.SMEM),
            pl.BlockSpec(memory_space=pltpu.SMEM),
            pl.BlockSpec(memory_space=pltpu.VMEM),
        ],
        out_specs=[
            pl.BlockSpec(memory_space=pltpu.VMEM),
            pl.BlockSpec(memory_space=pltpu.SMEM),
        ],
        out_shape=[
            jax.ShapeDtypeStruct((parts, waves // half, pairs, 2 * half), jnp.float32),
            jax.ShapeDtypeStruct((waves,), jnp.int32),
        ],
        scratch_shapes=[pltpu.VMEM((waves, bands), jnp.float32)],
        compiler_params=params(),
        name="sort",
    )(rank, key, wave)


def lane_gather(values, index):
    numbers = lax.GatherDimensionNumbers(
        offset_dims=(),
        collapsed_slice_dims=(1,),
        start_index_map=(1,),
        operand_batching_dims=(0,),
        start_indices_batching_dims=(0,),
    )
    return lax.gather(
        values,
        index[..., None],
        numbers,
        slice_sizes=(1, 1),
        mode=lax.GatherScatterMode.PROMISE_IN_BOUNDS,
    )


def grid_kernel(
    block_ref,
    first_ref,
    last_ref,
    code_ref,
    slot_row_ref,
    slot_y_ref,
    potential_ref,
    left_ref,
    right_ref,
    compact_ref,
    out_ref,
    grid_ref,
    *,
    size,
    pitch,
    band_pitch,
):
    blocks, pairs, lanes = out_ref.shape
    half = lanes // 2
    rows = size * size
    shift = size.bit_length() - 1
    extra = pitch - size
    upper = lax.broadcasted_iota(jnp.int32, (pairs, lanes), 1) // half * half
    wide = math.gcd(rows, 64)

    def expand(group, carry):
        base = group * wide
        place = base + lax.shift_right_logical(base, shift) * extra
        for step in range(wide):
            row = base + step
            block = block_ref[row]
            code = jnp.broadcast_to(code_ref[pl.ds(row, 1), :], (pairs, lanes))
            index = (code & (half - 1)) | upper
            here = lane_gather(compact_ref[block], index)
            there = lane_gather(compact_ref[block + 1], index)
            value = jnp.where(code < half, here, there)
            value = jnp.where(code >= 0, value, 0.0)
            grid_ref[pl.ds(place + step, pairs, stride=band_pitch), :] = value
        return carry

    lax.fori_loop(0, rows // wide, expand, 0)

    left = left_ref[...]
    right = right_ref[...]

    def apply_left(value):
        high, low = split_bf16(value)
        both = dot32(left, jnp.concatenate([high, low], axis=0))
        return both[:size, :] + both[size:, :]

    def apply_right(value):
        high, low = split_bf16(value)
        both = dot32(jnp.concatenate([high, low], axis=1), right)
        return both[:, :lanes] + both[:, lanes:]

    many = 8

    chains = max(1, math.gcd(size // many, 4))
    groups = size // (many * chains)

    def planes(turn, carry):
        base = turn // groups * band_pitch
        offset = turn % groups * (many * chains * pitch)
        for chain in range(chains):
            starts = [
                pl.multiple_of(base + offset + (chain * many + index) * pitch, 8)
                for index in range(many)
            ]
            field = jnp.concatenate([grid_ref[pl.ds(s, size), :] for s in starts], axis=1)
            field = apply_left(field)
            field = jnp.concatenate(
                [field[:, index * lanes : (index + 1) * lanes] for index in range(many)], axis=0
            )
            field = apply_right(field)
            for index, s in enumerate(starts):
                grid_ref[pl.ds(s, size), :] = field[index * size : (index + 1) * size, :]
        return carry

    def columns(turn, carry):
        along = turn % groups * (many * chains)
        base = turn // groups * band_pitch + along
        for chain in range(chains):
            spots = [chain * many + index for index in range(many)]
            field = jnp.concatenate(
                [grid_ref[pl.ds(base + spot, size, stride=pitch), :] for spot in spots], axis=1
            )
            field = apply_left(field)
            weight = jnp.concatenate(
                [
                    potential_ref[pl.ds(pl.multiple_of((along + spot) * size, size), size), :]
                    for spot in spots
                ],
                axis=1,
            )
            field = apply_left(field * weight)
            for index, spot in enumerate(spots):
                grid_ref[pl.ds(base + spot, size, stride=pitch), :] = field[
                    :, index * lanes : (index + 1) * lanes
                ]
        return carry

    turns = pairs * groups
    lax.fori_loop(0, turns, planes, 0)
    lax.fori_loop(0, turns, columns, 0)
    lax.fori_loop(0, turns, planes, 0)

    visits = 12

    def visit(row, wanted, index, value):
        source = row + lax.shift_right_logical(row, shift) * extra
        here = lane_gather(grid_ref[pl.ds(source, pairs, stride=band_pitch), :], index)
        return jnp.where(wanted == row, here, value)

    def slots(block):
        wanted = jnp.broadcast_to(slot_row_ref[pl.ds(block, 1), :], (pairs, lanes))
        index = jnp.broadcast_to(slot_y_ref[pl.ds(block, 1), :], (pairs, lanes))
        return wanted, index

    together = math.gcd(blocks, 8)

    def collect(group, carry):
        longest = 0
        for step in range(together):
            block = group * together + step
            wanted, index = slots(block)
            first = first_ref[block]
            value = jnp.zeros((pairs, lanes), jnp.float32)
            for number in range(visits):
                value = visit(first + number, wanted, index, value)
            out_ref[block] = value
            longest = jnp.maximum(longest, last_ref[block] - first)

        @pl.when(longest >= visits)
        def _():
            for step in range(together):
                block = group * together + step
                wanted, index = slots(block)
                first = first_ref[block]
                out_ref[block] = lax.fori_loop(
                    first + visits,
                    last_ref[block] + 1,
                    lambda row, value: visit(row, wanted, index, value),
                    out_ref[block],
                )

        return carry

    lax.fori_loop(0, blocks // together, collect, 0)


def grid_call(block_of, first, last, code, slot_row, slot_y, potential, left, right, compact, size):
    _, pairs, lanes = compact.shape
    blocks = first.shape[0]
    pitch = size + 8
    band_pitch = size * pitch + 8
    smem = pl.BlockSpec(memory_space=pltpu.SMEM)
    vmem = pl.BlockSpec(memory_space=pltpu.VMEM)
    points = 2 * pairs * size**3
    return pl.pallas_call(
        functools.partial(grid_kernel, size=size, pitch=pitch, band_pitch=band_pitch),
        in_specs=[smem] * 3 + [vmem] * 7,
        out_specs=vmem,
        out_shape=jax.ShapeDtypeStruct((blocks, pairs, lanes), jnp.float32),
        scratch_shapes=[pltpu.VMEM((pairs * band_pitch + 16, lanes), jnp.float32)],
        compiler_params=params(),
        cost_estimate=pl.CostEstimate(
            flops=36 * size * points, bytes_accessed=4 * points, transcendentals=0
        ),
        name="grid",
    )(block_of, first, last, code, slot_row, slot_y, potential, left, right, compact)


def finish_kernel(rank_ref, back_ref, muffin_ref, all_ref, out_ref, sub_ref, rows_ref):
    block, bands = out_ref.shape
    parts, _, _, lanes = back_ref.shape
    half = lanes // 2
    turn = pl.program_id(0)

    @pl.when(turn == 0)
    def _():
        sub_ref[...] = jnp.zeros_like(sub_ref)

        def order(tile, carry):
            start = pl.multiple_of(tile * lanes, lanes)
            pieces = []
            for part in range(parts):
                even = back_ref[part, 2 * tile]
                odd = back_ref[part, 2 * tile + 1]
                pieces.append(jnp.concatenate([even[:, :half], odd[:, :half]], axis=1))
                pieces.append(jnp.concatenate([even[:, half:], odd[:, half:]], axis=1))
            rows_ref[pl.ds(start, lanes), :] = jnp.concatenate(pieces, axis=0).T
            return carry

        lax.fori_loop(0, rows_ref.shape[0] // lanes, order, 0)

    first = turn * block

    def place(index, carry):
        out_ref[pl.ds(index, 1), :] = rows_ref[pl.ds(rank_ref[first + index], 1), :]
        return carry

    lax.fori_loop(0, block, place, 0, unroll=32)
    applied = muffin_ref[...] + out_ref[...].T
    out_ref[...] = applied.T
    high, low = split_bf16(applied)
    all_high, all_low = split_bf16(all_ref[...])
    main = dot32(jnp.concatenate([high, low], axis=0), all_high)
    sub_ref[...] += main[:bands, :] + main[bands:, :] + dot32(high, all_low)


def finish_call(rank, back, muffin, columns):
    bands, waves = muffin.shape
    total = columns.shape[1]
    block = math.gcd(waves, 512)
    return pl.pallas_call(
        finish_kernel,
        grid=(waves // block,),
        in_specs=[
            pl.BlockSpec(memory_space=pltpu.SMEM),
            pl.BlockSpec(back.shape, lambda i: (0, 0, 0, 0)),
            pl.BlockSpec((bands, block), lambda i: (0, i)),
            pl.BlockSpec((block, total), lambda i: (i, 0)),
        ],
        out_specs=[
            pl.BlockSpec((block, bands), lambda i: (i, 0)),
            pl.BlockSpec((bands, total), lambda i: (0, 0)),
        ],
        out_shape=[
            jax.ShapeDtypeStruct((waves, bands), jnp.float32),
            jax.ShapeDtypeStruct((bands, total), jnp.float32),
        ],
        scratch_shapes=[pltpu.VMEM((waves, bands), jnp.float32)],
        compiler_params=params("arbitrary"),
        name="finish",
    )(rank, back, muffin, columns)


def exchange(array):
    return lax.all_to_all(array, "pw", split_axis=0, concat_axis=0, tiled=True)


def round_high(value):
    return lax.reduce_precision(value, 8, 7)


def interstitial_tables(size):
    table = cas_matrix(size)
    high = round_high(table)
    low = round_high(table - high)
    zero = jnp.zeros_like(table)
    left = jnp.concatenate(
        [jnp.concatenate([high, high], axis=1), jnp.concatenate([low, zero], axis=1)], axis=0
    )

    def twice(block):
        return jnp.concatenate(
            [jnp.concatenate([block, zero], axis=1), jnp.concatenate([zero, block], axis=1)], axis=0
        )

    right = jnp.concatenate(
        [
            jnp.concatenate([twice(high), twice(low)], axis=1),
            jnp.concatenate([twice(high), jnp.zeros((2 * size, 2 * size))], axis=1),
        ],
        axis=0,
    )
    return left.astype(jnp.bfloat16), right.astype(jnp.bfloat16)


def whole_step(wave_coeffs, miller, atom_types, positions, sphere_radii, h_blocks, potential):
    pw_count = lax.axis_size("pw")
    pw_index = lax.axis_index("pw")
    local_waves, local_bands = wave_coeffs.shape
    size = potential.shape[1]
    kinds, funcs_each = h_blocks.shape[:2]
    atom_total = atom_types.shape[0]
    factor = NPW ** (-0.5)
    miller_float = miller.astype(jnp.float32)
    kinetic = jnp.sum(miller_float * miller_float, axis=0) / 1536.0
    planes_each = size // pw_count
    lines = planes_each * size

    wrapped = jnp.mod(miller, size)
    line = (wrapped[2] - pw_index * planes_each) * size + wrapped[0]
    key = line * size + wrapped[1]
    rank = jnp.sum((key[:, None] < key[None, :]).astype(jnp.int32), axis=0)
    turned = jnp.transpose(potential, (0, 2, 1))
    pieces = [
        turned.reshape(-1),
        line.astype(jnp.float32),
        wrapped[1].astype(jnp.float32),
    ]
    cuts = np.cumsum([piece.shape[0] for piece in pieces])
    known = lax.all_gather(jnp.concatenate(pieces), "pw", axis=0, tiled=False)

    send, sorted_key = sort_call(rank, key, wave_coeffs, pw_count, size)
    blocks_each, pairs, lanes = send.shape[1:]
    keys = sorted_key.astype(jnp.float32).reshape(1, -1, pairs, lanes)
    send = jnp.concatenate([send, jnp.broadcast_to(keys, (pw_count,) + keys.shape[1:])], axis=1)
    compact = exchange(send)

    spheres, matching_table, phase = sphere_call(
        atom_types, miller, positions, sphere_radii, wave_coeffs, kinds, funcs_each, 2.0 / size
    )
    spheres = lax.psum(spheres, "pw").reshape(atom_total, funcs_each, local_bands)
    onehot = (atom_types[:, None] == jnp.arange(kinds, dtype=jnp.int32)[None, :]).astype(
        jnp.float32
    )
    chosen = jnp.einsum("at,tfk->afk", onehot, h_blocks, precision=PRECISE)

    wave_again, known = lax.optimization_barrier((wave_coeffs, known))
    columns = lax.all_gather(wave_again, "band", axis=1, tiled=True)

    field = known[:, : cuts[0]].reshape(size * size, size)
    field = jnp.concatenate([field, field], axis=1)
    all_lines = known[:, cuts[0] : cuts[1]].astype(jnp.int32)
    all_across = known[:, cuts[1] : cuts[2]].astype(jnp.int32)
    line_ids = jnp.arange(lines, dtype=jnp.int32)
    across = jnp.arange(size, dtype=jnp.int32)
    filled = jnp.einsum(
        "plg,pgy->ply",
        (all_lines[:, None, :] == line_ids[None, :, None]).astype(jnp.bfloat16),
        (all_across[:, :, None] == across[None, None, :]).astype(jnp.bfloat16),
        preferred_element_type=jnp.float32,
    )
    before = (across[:, None] < across[None, :]).astype(jnp.bfloat16)
    ahead = jnp.einsum(
        "ply,yv->plv", filled.astype(jnp.bfloat16), before, preferred_element_type=jnp.float32
    )
    earlier = (line_ids[:, None] < line_ids[None, :]).astype(jnp.bfloat16)
    starts = jnp.einsum(
        "pl,lm->pm",
        jnp.sum(filled, axis=2).astype(jnp.bfloat16),
        earlier,
        preferred_element_type=jnp.float32,
    ).astype(jnp.int32)
    starts = starts + jnp.arange(pw_count, dtype=jnp.int32)[:, None] * local_waves
    block_of = jnp.minimum(starts // size, pw_count * blocks_each - 2)
    codes = ahead.astype(jnp.int32) + (starts - block_of * size)[:, :, None]
    codes = jnp.where(filled > 0.5, codes, -1).reshape(size * size, size)
    codes = jnp.concatenate([codes, codes], axis=1)

    all_keys = compact[:, blocks_each:].astype(jnp.int32).reshape(pw_count, -1)
    offsets = jnp.arange(pw_count, dtype=jnp.int32)[:, None] * (lines * size)
    all_keys = (all_keys + offsets).reshape(-1, size)
    slot_row = all_keys // size
    slot_y = all_keys % size
    compact = compact[:, :blocks_each].reshape(-1, pairs, lanes)
    left, right = interstitial_tables(size)
    back = grid_call(
        block_of.reshape(-1),
        slot_row[:, 0],
        slot_row[:, -1],
        codes,
        jnp.concatenate([slot_row, slot_row], axis=1),
        jnp.concatenate([slot_y, slot_y + size], axis=1),
        field,
        left,
        right,
        compact,
        size,
    )
    back = exchange(back.reshape(pw_count, blocks_each, pairs, lanes))
    applied = jnp.einsum("akb,afk->baf", spheres, chosen, precision=PRECISE)
    muffin = muffin_call(
        atom_types, matching_table, phase, applied.reshape(local_bands, -1), kinetic, wave_coeffs
    )
    h_applied, partial = finish_call(rank, back, muffin, columns)
    partial = jnp.transpose(partial) * factor
    rows_each = partial.shape[0] // pw_count
    gathered = exchange(partial.reshape(pw_count, rows_each, local_bands))
    return (h_applied, jnp.sum(gathered, axis=0))


def solution(mesh):
    in_specs = (P("pw", "band"), P(None, "pw"), P(), P(), P(), P(), P("pw", None, None))
    out_specs = (P("pw", "band"), P("pw", "band"))
    return jax.shard_map(
        whole_step, mesh=mesh, in_specs=in_specs, out_specs=out_specs, check_vma=False
    )
```

```python
import functools
import math

import jax
import jax.numpy as jnp
import numpy as np
from jax import lax
from jax.experimental import pallas as pl
from jax.experimental.pallas import tpu as pltpu
from jax.sharding import PartitionSpec as P

NPW = 32768


PRECISE = lax.Precision.HIGHEST


def double_factorial(value):
    result = 1
    while value > 1:
        result = result * value
        value = value - 2
    return float(result)


def bessel_table(argument, count):
    safe = jnp.maximum(argument, 1.0)
    upward = [jnp.sin(safe) / safe, jnp.sin(safe) / (safe * safe) - jnp.cos(safe) / safe]
    for degree in range(1, count - 1):
        upward.append((2 * degree + 1) / safe * upward[degree] - upward[degree - 1])
    half_square = -0.5 * argument * argument
    power = jnp.ones_like(argument)
    columns = []
    for degree in range(count):
        term = jnp.ones_like(argument)
        total = jnp.ones_like(argument)
        for index in range(1, 17):
            term = term * half_square / float(index * (2 * degree + 2 * index + 1))
            total = total + term
        series = power * total / double_factorial(2 * degree + 1)
        power = power * argument
        columns.append(jnp.where(argument > degree + 1, upward[degree], series))
    return columns


def harmonic_table(unit, count):
    along_x, along_y, along_z = (unit[0], unit[1], unit[2])
    ones = jnp.ones_like(along_z)
    cosines = [ones]
    sines = [jnp.zeros_like(along_z)]
    for azimuth in range(1, count):
        cosines.append(along_x * cosines[-1] - along_y * sines[-1])
        sines.append(along_x * sines[-2 + 1] + along_y * cosines[-2])
    legendre = {}
    for azimuth in range(count):
        legendre[azimuth, azimuth] = double_factorial(2 * azimuth - 1) * ones
        if azimuth + 1 < count:
            legendre[azimuth + 1, azimuth] = (
                (2 * azimuth + 1) * along_z * legendre[azimuth, azimuth]
            )
        for degree in range(azimuth + 2, count):
            legendre[degree, azimuth] = (
                (2 * degree - 1) * along_z * legendre[degree - 1, azimuth]
                - (degree + azimuth - 1) * legendre[degree - 2, azimuth]
            ) / float(degree - azimuth)
    columns = []
    for degree in range(count):
        for signed in range(-degree, degree + 1):
            azimuth = abs(signed)
            weight = math.sqrt(
                (2 * degree + 1)
                * math.factorial(degree - azimuth)
                / (4.0 * math.pi * math.factorial(degree + azimuth))
            )
            if azimuth > 0:
                weight = weight * math.sqrt(2.0)
            circle = cosines[azimuth] if signed >= 0 else sines[azimuth]
            columns.append(weight * legendre[degree, azimuth] * circle)
    return columns


def cas_matrix(grid_size):
    across = jnp.arange(grid_size, dtype=jnp.int32)
    phase = across[:, None] * across[None, :] % grid_size
    angle = 2.0 * math.pi / grid_size * phase.astype(jnp.float32)
    return (jnp.cos(angle) + jnp.sin(angle)) / math.sqrt(grid_size)


def split_bf16(value):
    high = value.astype(jnp.bfloat16)
    low = (value - high.astype(jnp.float32)).astype(jnp.bfloat16)
    return high, low


def dot32(left, right):
    return jnp.dot(left, right, preferred_element_type=jnp.float32)


def params(*semantics):
    return pltpu.CompilerParams(
        dimension_semantics=semantics or None, vmem_limit_bytes=56 * 1024 * 1024
    )


def fill_matching(types_ref, table_ref, phase_ref, high_ref, low_ref):
    atoms = phase_ref.shape[0]
    funcs = table_ref.shape[1]

    def one(atom, carry):
        tile = table_ref[types_ref[atom]] * phase_ref[pl.ds(atom, 1), :]
        high, low = split_bf16(tile)
        start = pl.multiple_of(atom * funcs, funcs)
        high_ref[pl.ds(start, funcs), :] = high
        low_ref[pl.ds(start, funcs), :] = low
        return carry

    lax.fori_loop(0, atoms, one, 0, unroll=4)


def fill_tables(miller_ref, places_ref, radii_ref, table_ref, phase_ref, angular_ref, spacing):
    kinds, funcs, _ = table_ref.shape
    degree_count = math.isqrt(funcs)
    miller = miller_ref[...].astype(jnp.float32)
    along = [miller[axis : axis + 1, :] for axis in range(3)]
    norm = jnp.sqrt(along[0] * along[0] + along[1] * along[1] + along[2] * along[2])
    scale = jnp.maximum(norm, 1.0)
    for index, column in enumerate(harmonic_table([part / scale for part in along], degree_count)):
        angular_ref[index : index + 1, :] = column
    argument = radii_ref[...] * norm * spacing
    weight = 4.0 * math.pi * NPW ** (-0.5)
    for degree, column in enumerate(bessel_table(argument, degree_count)):
        first, last = degree * degree, (degree + 1) * (degree + 1)
        rows = angular_ref[first:last, :]
        for kind in range(kinds):
            table_ref[kind, first:last, :] = rows * (column[kind : kind + 1, :] * weight)
    places = places_ref[...]
    turns = sum(places[:, axis : axis + 1] * along[axis] for axis in range(3))
    angle = 2.0 * math.pi * (turns - jnp.round(turns))
    phase_ref[...] = jnp.cos(angle) + jnp.sin(angle)


def sphere_kernel(
    types_ref,
    miller_ref,
    places_ref,
    radii_ref,
    wave_ref,
    out_ref,
    table_ref,
    phase_ref,
    angular_ref,
    high_ref,
    low_ref,
    *,
    spacing,
):
    bands = wave_ref.shape[1]

    @pl.when(pl.program_id(0) == 0)
    def _():
        out_ref[...] = jnp.zeros_like(out_ref)

    fill_tables(miller_ref, places_ref, radii_ref, table_ref, phase_ref, angular_ref, spacing)
    fill_matching(types_ref, table_ref, phase_ref, high_ref, low_ref)
    wave_high, wave_low = split_bf16(wave_ref[...])
    both = jnp.concatenate([wave_high, wave_low], axis=1)
    rows = out_ref.shape[0]
    step = math.gcd(rows, 512)
    for first in range(0, rows, step):
        main = dot32(high_ref[first : first + step, :], both)
        rest = dot32(low_ref[first : first + step, :], wave_high)
        out_ref[first : first + step, :] += main[:, :bands] + main[:, bands:] + rest


def sphere_call(types, miller, positions, radii, wave, kinds, funcs, spacing):
    waves, bands = wave.shape
    atoms = positions.shape[1]
    block = math.gcd(waves, 1024)
    rows = atoms * funcs
    return pl.pallas_call(
        functools.partial(sphere_kernel, spacing=spacing),
        grid=(waves // block,),
        in_specs=[
            pl.BlockSpec(memory_space=pltpu.SMEM),
            pl.BlockSpec((3, block), lambda i: (0, i)),
            pl.BlockSpec((atoms, 3), lambda i: (0, 0)),
            pl.BlockSpec((kinds, 1), lambda i: (0, 0)),
            pl.BlockSpec((block, bands), lambda i: (i, 0)),
        ],
        out_specs=[
            pl.BlockSpec((rows, bands), lambda i: (0, 0)),
            pl.BlockSpec((kinds, funcs, block), lambda i: (0, 0, i)),
            pl.BlockSpec((atoms, block), lambda i: (0, i)),
        ],
        out_shape=[
            jax.ShapeDtypeStruct((rows, bands), jnp.float32),
            jax.ShapeDtypeStruct((kinds, funcs, waves), jnp.float32),
            jax.ShapeDtypeStruct((atoms, waves), jnp.float32),
        ],
        scratch_shapes=[
            pltpu.VMEM((funcs, block), jnp.float32),
            pltpu.VMEM((rows, block), jnp.bfloat16),
            pltpu.VMEM((rows, block), jnp.bfloat16),
        ],
        compiler_params=params("arbitrary"),
        cost_estimate=pl.CostEstimate(
            flops=6 * waves * rows * bands, bytes_accessed=8 * waves * bands, transcendentals=0
        ),
        name="sphere",
    )(types, miller, positions.T, radii[:, None], wave)


def muffin_kernel(
    types_ref,
    table_ref,
    phase_ref,
    sphere_ref,
    kinetic_ref,
    wave_ref,
    out_ref,
    high_ref,
    low_ref,
):
    bands = out_ref.shape[0]
    fill_matching(types_ref, table_ref, phase_ref, high_ref, low_ref)
    high, low = split_bf16(sphere_ref[...])
    main = dot32(jnp.concatenate([high, low], axis=0), high_ref[...])
    rest = dot32(high, low_ref[...])
    kinetic = kinetic_ref[...] * wave_ref[...].T
    out_ref[...] = main[:bands, :] + main[bands:, :] + rest + kinetic


def muffin_call(types, table, phase, sphere, kinetic, wave):
    kinds, funcs, waves = table.shape
    atoms = phase.shape[0]
    bands, rows = sphere.shape
    block = math.gcd(waves, 1024)
    return pl.pallas_call(
        muffin_kernel,
        grid=(waves // block,),
        in_specs=[
            pl.BlockSpec(memory_space=pltpu.SMEM),
            pl.BlockSpec((kinds, funcs, block), lambda i: (0, 0, i)),
            pl.BlockSpec((atoms, block), lambda i: (0, i)),
            pl.BlockSpec((bands, rows), lambda i: (0, 0)),
            pl.BlockSpec((1, block), lambda i: (0, i)),
            pl.BlockSpec((block, bands), lambda i: (i, 0)),
        ],
        out_specs=pl.BlockSpec((bands, block), lambda i: (0, i)),
        out_shape=jax.ShapeDtypeStruct((bands, waves), jnp.float32),
        scratch_shapes=[
            pltpu.VMEM((rows, block), jnp.bfloat16),
            pltpu.VMEM((rows, block), jnp.bfloat16),
        ],
        compiler_params=params("arbitrary"),
        cost_estimate=pl.CostEstimate(
            flops=6 * waves * rows * bands, bytes_accessed=8 * waves * bands, transcendentals=0
        ),
        name="muffin",
    )(types, table, phase, sphere, kinetic[None, :], wave)


def sort_kernel(rank_ref, key_ref, wave_ref, send_ref, sorted_ref, rows_ref):
    waves, _ = wave_ref.shape
    parts, _, pairs, lanes = send_ref.shape
    half = lanes // 2

    def place(index, carry):
        target = rank_ref[index]
        rows_ref[pl.ds(target, 1), :] = wave_ref[pl.ds(index, 1), :]
        sorted_ref[target] = key_ref[index]
        return carry

    lax.fori_loop(0, waves, place, 0, unroll=32)

    def turn(tile, carry):
        start = pl.multiple_of(tile * lanes, lanes)
        turned = rows_ref[pl.ds(start, lanes), :].T
        for part in range(parts):
            first = part * 2 * pairs
            top = turned[first : first + pairs, :]
            low = turned[first + pairs : first + 2 * pairs, :]
            send_ref[part, 2 * tile] = jnp.concatenate([top[:, :half], low[:, :half]], axis=1)
            send_ref[part, 2 * tile + 1] = jnp.concatenate([top[:, half:], low[:, half:]], axis=1)
        return carry

    lax.fori_loop(0, waves // lanes, turn, 0)


def sort_call(rank, key, wave, parts, half):
    waves, bands = wave.shape
    pairs = bands // parts // 2
    stored = waves // half + waves // (pairs * 2 * half)
    return pl.pallas_call(
        sort_kernel,
        in_specs=[
            pl.BlockSpec(memory_space=pltpu.SMEM),
            pl.BlockSpec(memory_space=pltpu.SMEM),
            pl.BlockSpec(memory_space=pltpu.VMEM),
        ],
        out_specs=[
            pl.BlockSpec(memory_space=pltpu.VMEM),
            pl.BlockSpec(memory_space=pltpu.SMEM),
        ],
        out_shape=[
            jax.ShapeDtypeStruct((parts, stored, pairs, 2 * half), jnp.float32),
            jax.ShapeDtypeStruct((waves,), jnp.int32),
        ],
        scratch_shapes=[pltpu.VMEM((waves, bands), jnp.float32)],
        compiler_params=params(),
        name="sort",
    )(rank, key, wave)


def lane_gather(values, index):
    numbers = lax.GatherDimensionNumbers(
        offset_dims=(),
        collapsed_slice_dims=(1,),
        start_index_map=(1,),
        operand_batching_dims=(0,),
        start_indices_batching_dims=(0,),
    )
    return lax.gather(
        values,
        index[..., None],
        numbers,
        slice_sizes=(1, 1),
        mode=lax.GatherScatterMode.PROMISE_IN_BOUNDS,
    )


def grid_kernel(
    window_ref,
    deep_ref,
    first_ref,
    last_ref,
    code_ref,
    slot_row_ref,
    slot_y_ref,
    potential_ref,
    left_ref,
    right_ref,
    compact_ref,
    out_ref,
    grid_ref,
    windows_ref,
    *,
    size,
    pitch,
    band_pitch,
    wide,
):
    blocks, pairs, lanes = out_ref.shape
    half = lanes // 2
    rows = size * size
    shift = size.bit_length() - 1
    extra = pitch - size
    upper = lax.broadcasted_iota(jnp.int32, (pairs, lanes), 1) // half * half
    parts, _, _, _ = compact_ref.shape
    each = blocks // parts
    inner = lax.broadcasted_iota(jnp.int32, (pairs, lanes), 1) % half
    steps = math.gcd(each, 16)

    def widen(part, carry):
        following = jnp.minimum(part + 1, parts - 1)

        def some(group, carry):
            first = group * steps
            for step in range(steps):
                block = compact_ref[part, first + step]
                if step + 1 < steps:
                    after = compact_ref[part, first + step + 1]
                else:
                    inside = first + steps < each
                    after = compact_ref[
                        jnp.where(inside, part, following), jnp.where(inside, first + steps, 0)
                    ]
                mixed = jnp.where(
                    inner < half // 2,
                    pltpu.roll(block, lanes - half // 2, 1),
                    pltpu.roll(after, half // 2, 1),
                )
                spot = 2 * (part * each + first + step)
                windows_ref[spot] = block
                windows_ref[spot + 1] = mixed
            return carry

        return lax.fori_loop(0, each // steps, some, carry)

    lax.fori_loop(0, parts, widen, 0)

    def expand(group, carry):
        base = group * wide
        place = base + lax.shift_right_logical(base, shift) * extra

        @pl.when(deep_ref[group] == 0)
        def _():
            for step in range(wide):
                row = base + step
                code = jnp.broadcast_to(code_ref[pl.ds(row, 1), :], (pairs, lanes))
                index = (code & (half - 1)) | upper
                value = lane_gather(windows_ref[window_ref[row]], index)
                value = jnp.where(code >= 0, value, 0.0)
                grid_ref[pl.ds(place + step, pairs, stride=band_pitch), :] = value

        @pl.when(deep_ref[group] != 0)
        def _():
            def one(step, carry):
                row = base + step
                code = jnp.broadcast_to(code_ref[pl.ds(row, 1), :], (pairs, lanes))
                index = (code & (half - 1)) | upper
                window = window_ref[row]
                later = jnp.minimum(window + 2, 2 * blocks - 1)
                here = lane_gather(windows_ref[window], index)
                there = lane_gather(windows_ref[later], index)
                value = jnp.where(code < half, here, there)
                value = jnp.where(code >= 0, value, 0.0)
                grid_ref[pl.ds(place + step, pairs, stride=band_pitch), :] = value
                return carry

            lax.fori_loop(0, wide, one, 0)

        return carry

    lax.fori_loop(0, rows // wide, expand, 0)

    left = left_ref[...]
    right = right_ref[...]

    def apply_left(value):
        high, low = split_bf16(value)
        both = dot32(left, jnp.concatenate([high, low], axis=0))
        return both[:size, :] + both[size:, :]

    def apply_right(value):
        high, low = split_bf16(value)
        both = dot32(jnp.concatenate([high, low], axis=1), right)
        return both[:, :lanes] + both[:, lanes:]

    many = 8

    chains = max(1, math.gcd(size // many, 4))
    groups = size // (many * chains)

    def planes(turn, carry):
        base = turn // groups * band_pitch
        offset = turn % groups * (many * chains * pitch)
        for chain in range(chains):
            starts = [
                pl.multiple_of(base + offset + (chain * many + index) * pitch, 8)
                for index in range(many)
            ]
            field = jnp.concatenate([grid_ref[pl.ds(s, size), :] for s in starts], axis=1)
            field = apply_left(field)
            field = jnp.concatenate(
                [field[:, index * lanes : (index + 1) * lanes] for index in range(many)], axis=0
            )
            field = apply_right(field)
            for index, s in enumerate(starts):
                grid_ref[pl.ds(s, size), :] = field[index * size : (index + 1) * size, :]
        return carry

    def columns(turn, carry):
        along = turn % groups * (many * chains)
        base = turn // groups * band_pitch + along
        for chain in range(chains):
            spots = [chain * many + index for index in range(many)]
            field = jnp.concatenate(
                [grid_ref[pl.ds(base + spot, size, stride=pitch), :] for spot in spots], axis=1
            )
            field = apply_left(field)
            weight = jnp.concatenate(
                [
                    potential_ref[pl.ds(pl.multiple_of((along + spot) * size, size), size), :]
                    for spot in spots
                ],
                axis=1,
            )
            field = apply_left(field * weight)
            for index, spot in enumerate(spots):
                grid_ref[pl.ds(base + spot, size, stride=pitch), :] = field[
                    :, index * lanes : (index + 1) * lanes
                ]
        return carry

    turns = pairs * groups
    lax.fori_loop(0, turns, planes, 0)
    lax.fori_loop(0, turns, columns, 0)
    lax.fori_loop(0, turns, planes, 0)

    visits = 12

    def visit(row, wanted, index, value):
        source = row + lax.shift_right_logical(row, shift) * extra
        here = lane_gather(grid_ref[pl.ds(source, pairs, stride=band_pitch), :], index)
        return jnp.where(wanted == row, here, value)

    def slots(block):
        wanted = jnp.broadcast_to(slot_row_ref[pl.ds(block, 1), :], (pairs, lanes))
        index = jnp.broadcast_to(slot_y_ref[pl.ds(block, 1), :], (pairs, lanes))
        return wanted, index

    together = math.gcd(blocks, 8)

    def collect(group, carry):
        longest = 0
        for step in range(together):
            block = group * together + step
            wanted, index = slots(block)
            first = first_ref[block]
            value = jnp.zeros((pairs, lanes), jnp.float32)
            for number in range(visits):
                value = visit(first + number, wanted, index, value)
            out_ref[block] = value
            longest = jnp.maximum(longest, last_ref[block] - first)

        @pl.when(longest >= visits)
        def _():
            for step in range(together):
                block = group * together + step
                wanted, index = slots(block)
                first = first_ref[block]
                out_ref[block] = lax.fori_loop(
                    first + visits,
                    last_ref[block] + 1,
                    lambda row, value: visit(row, wanted, index, value),
                    out_ref[block],
                )

        return carry

    lax.fori_loop(0, blocks // together, collect, 0)


def grid_call(window, deep, first, last, code, slot_row, slot_y, field, left, right, compact, size):
    _, _, pairs, lanes = compact.shape
    blocks = first.shape[0]
    pitch = size + 8
    band_pitch = size * pitch + 8
    smem = pl.BlockSpec(memory_space=pltpu.SMEM)
    vmem = pl.BlockSpec(memory_space=pltpu.VMEM)
    points = 2 * pairs * size**3
    return pl.pallas_call(
        functools.partial(
            grid_kernel,
            size=size,
            pitch=pitch,
            band_pitch=band_pitch,
            wide=size * size // deep.shape[0],
        ),
        in_specs=[smem] * 4 + [vmem] * 7,
        out_specs=vmem,
        out_shape=jax.ShapeDtypeStruct((blocks, pairs, lanes), jnp.float32),
        scratch_shapes=[
            pltpu.VMEM((pairs * band_pitch + 16, lanes), jnp.float32),
            pltpu.VMEM((2 * blocks, pairs, lanes), jnp.float32),
        ],
        compiler_params=params(),
        cost_estimate=pl.CostEstimate(
            flops=36 * size * points, bytes_accessed=4 * points, transcendentals=0
        ),
        name="grid",
    )(window, deep, first, last, code, slot_row, slot_y, field, left, right, compact)


def prepare_kernel(known_ref, lanes_ref, rows_ref, code_ref, field_ref, *, waves, low_count, size):
    lanes = known_ref.shape[2]
    left_ids, right_ids = rows_ref.shape[0], lanes_ref.shape[0]
    field_rows = code_ref.shape[1] // 2
    wave_rows = waves // lanes
    part = pl.program_id(0)

    def onehot(first, count):
        ids = lax.broadcasted_iota(jnp.int32, (count, lanes), 0).astype(jnp.float32)
        return jnp.concatenate(
            [
                jnp.where(known_ref[0, row : row + 1, :] == ids, 1.0, 0.0).astype(jnp.bfloat16)
                for row in range(first, first + wave_rows)
            ],
            axis=1,
        )

    filled = lax.dot_general(
        onehot(field_rows, left_ids),
        onehot(field_rows + wave_rows, right_ids),
        (((1,), (1,)), ((), ())),
        preferred_element_type=jnp.float32,
    )
    sums = dot32(filled.astype(jnp.bfloat16), lanes_ref[...])
    ahead = sums[:, :right_ids]
    counts = jnp.concatenate(
        [sums[:, index * right_ids : (index + 1) * right_ids] for index in (1, 2, 3)], axis=0
    )
    start = dot32(rows_ref[...], counts.astype(jnp.bfloat16)).astype(jnp.int32) + part * waves
    code = ahead.astype(jnp.int32) + (start & (size // 2 - 1))
    code = jnp.where(filled > 0.5, code, -1)
    for low in range(low_count):
        piece = code[:, low * size : (low + 1) * size]
        piece = jnp.concatenate([piece, piece], axis=1)
        for high in range(left_ids // size):
            first = (high * low_count + low) * size
            code_ref[0, first : first + size, :] = piece[high * size : (high + 1) * size, :]
    field = known_ref[0, :field_rows, :]
    for side in range(2):
        half = field[:, side * size : (side + 1) * size]
        field_ref[0, pl.ds(side, field_rows, stride=2), :] = jnp.concatenate([half, half], axis=1)


def prepare_call(known, waves, planes_each, size):
    parts, stored, lanes = known.shape
    low_count = math.gcd(planes_each, 4)
    high_count = planes_each // low_count
    lines = planes_each * size
    eye = np.eye(low_count)
    square = np.ones((size, size))
    before = np.triu(square, 1)
    lanes_table = np.concatenate(
        [
            np.kron(eye, before),
            np.kron(eye, square),
            np.kron(np.triu(np.ones((low_count, low_count)), 1), square),
            np.kron(np.ones((low_count, low_count)), square),
        ],
        axis=1,
    )
    eye = np.eye(high_count)
    rows_table = np.concatenate(
        [
            np.kron(eye, before.T),
            np.kron(eye, square),
            np.kron(np.tril(np.ones((high_count, high_count)), -1), square),
        ],
        axis=1,
    )
    return pl.pallas_call(
        functools.partial(prepare_kernel, waves=waves, low_count=low_count, size=size),
        grid=(parts,),
        in_specs=[
            pl.BlockSpec((1, stored, lanes), lambda i: (i, 0, 0)),
            pl.BlockSpec(lanes_table.shape, lambda i: (0, 0)),
            pl.BlockSpec(rows_table.shape, lambda i: (0, 0)),
        ],
        out_specs=[pl.BlockSpec((1, lines, lanes), lambda i: (i, 0, 0))] * 2,
        out_shape=[
            jax.ShapeDtypeStruct((parts, lines, lanes), jnp.int32),
            jax.ShapeDtypeStruct((parts, lines, lanes), jnp.float32),
        ],
        compiler_params=params("arbitrary"),
        cost_estimate=pl.CostEstimate(
            flops=2 * parts * waves * lines * size, bytes_accessed=4 * parts * waves, transcendentals=0
        ),
        name="prepare",
    )(known, jnp.asarray(lanes_table, jnp.bfloat16), jnp.asarray(rows_table, jnp.bfloat16))


def finish_kernel(rank_ref, where_ref, back_ref, muffin_ref, *refs):
    *all_refs, out_ref, sub_ref, rows_ref = refs
    block, bands = out_ref.shape
    parts, _, _, lanes = back_ref.shape
    half = lanes // 2
    turn = pl.program_id(0)

    @pl.when(turn == 0)
    def _():
        sub_ref[...] = jnp.zeros_like(sub_ref)

        def order(tile, carry):
            start = pl.multiple_of(tile * lanes, lanes)
            pieces = []
            for part in range(parts):
                even = back_ref[part, 2 * tile]
                odd = back_ref[part, 2 * tile + 1]
                pieces.append(jnp.concatenate([even[:, :half], odd[:, :half]], axis=1))
                pieces.append(jnp.concatenate([even[:, half:], odd[:, half:]], axis=1))
            rows_ref[pl.ds(start, lanes), :] = jnp.concatenate(pieces, axis=0).T
            return carry

        lax.fori_loop(0, rows_ref.shape[0] // lanes, order, 0, unroll=4)

    first = turn * block

    def place(index, carry):
        out_ref[pl.ds(index, 1), :] = rows_ref[pl.ds(rank_ref[first + index], 1), :]
        return carry

    lax.fori_loop(0, block, place, 0, unroll=64)
    applied = muffin_ref[...] + out_ref[...].T
    out_ref[...] = applied.T
    high, low = split_bf16(applied)
    both = jnp.concatenate([high, low], axis=0)
    for shift, all_ref in enumerate(all_refs):
        all_high, all_low = split_bf16(all_ref[...])
        main = dot32(both, all_high)
        total = main[:bands, :] + main[bands:, :] + dot32(high, all_low)
        sub_ref[where_ref[shift]] += total

    @pl.when(turn == pl.num_programs(0) - 1)
    def _():
        for group in range(sub_ref.shape[0]):
            sub_ref[group] = sub_ref[group].T * NPW ** (-0.5)


def finish_call(rank, where, back, muffin, columns):
    bands, waves = muffin.shape
    groups = len(columns)
    block = math.gcd(waves, 2048)
    return pl.pallas_call(
        finish_kernel,
        grid=(waves // block,),
        in_specs=[
            pl.BlockSpec(memory_space=pltpu.SMEM),
            pl.BlockSpec(memory_space=pltpu.SMEM),
            pl.BlockSpec(back.shape, lambda i: (0, 0, 0, 0)),
            pl.BlockSpec((bands, block), lambda i: (0, i)),
        ]
        + [pl.BlockSpec((block, bands), lambda i: (i, 0))] * groups,
        out_specs=[
            pl.BlockSpec((block, bands), lambda i: (i, 0)),
            pl.BlockSpec((groups, bands, bands), lambda i: (0, 0, 0)),
        ],
        out_shape=[
            jax.ShapeDtypeStruct((waves, bands), jnp.float32),
            jax.ShapeDtypeStruct((groups, bands, bands), jnp.float32),
        ],
        scratch_shapes=[pltpu.VMEM((waves, bands), jnp.float32)],
        compiler_params=params("arbitrary"),
        name="finish",
    )(rank, where, back, muffin, *columns)


def exchange(array):
    return lax.all_to_all(array, "pw", split_axis=0, concat_axis=0, tiled=True)


def round_high(value):
    return lax.reduce_precision(value, 8, 7)


def interstitial_tables(size):
    table = cas_matrix(size)
    high = round_high(table)
    low = round_high(table - high)
    zero = jnp.zeros_like(table)
    left = jnp.concatenate(
        [jnp.concatenate([high, high], axis=1), jnp.concatenate([low, zero], axis=1)], axis=0
    )

    def twice(block):
        return jnp.concatenate(
            [jnp.concatenate([block, zero], axis=1), jnp.concatenate([zero, block], axis=1)], axis=0
        )

    right = jnp.concatenate(
        [
            jnp.concatenate([twice(high), twice(low)], axis=1),
            jnp.concatenate([twice(high), jnp.zeros((2 * size, 2 * size))], axis=1),
        ],
        axis=0,
    )
    return left.astype(jnp.bfloat16), right.astype(jnp.bfloat16)


def whole_step(wave_coeffs, miller, atom_types, positions, sphere_radii, h_blocks, potential):
    pw_count = lax.axis_size("pw")
    pw_index = lax.axis_index("pw")
    local_waves, local_bands = wave_coeffs.shape
    size = potential.shape[1]
    kinds, funcs_each = h_blocks.shape[:2]
    atom_total = atom_types.shape[0]
    miller_float = miller.astype(jnp.float32)
    kinetic = jnp.sum(miller_float * miller_float, axis=0) / 1536.0
    planes_each = size // pw_count
    lines = planes_each * size

    group_count = lax.axis_size("band")
    group = lax.axis_index("band")
    columns = [wave_coeffs]
    for shift in range(1, group_count):
        route = [(index, (index + shift) % group_count) for index in range(group_count)]
        columns.append(lax.ppermute(wave_coeffs, "band", route))
    where = jnp.mod(group - jnp.arange(group_count, dtype=jnp.int32), group_count)

    wrapped = jnp.mod(miller, size)
    line = (wrapped[2] - pw_index * planes_each) * size + wrapped[0]
    key = line * size + wrapped[1]
    rank = jnp.sum((key[:, None] < key[None, :]).astype(jnp.int32), axis=0)
    lanes = 2 * size
    low_count = math.gcd(planes_each, 4)
    plane = wrapped[2] - pw_index * planes_each
    starts = jnp.sum(
        (line[:, None] < jnp.arange(lines, dtype=jnp.int32)[None, :]).astype(jnp.int32), axis=0
    )
    pieces = [
        jnp.transpose(potential, (0, 2, 1)),
        (plane // low_count * size + wrapped[0]).astype(jnp.float32),
        (plane % low_count * size + wrapped[1]).astype(jnp.float32),
        starts.astype(jnp.float32),
    ]
    pieces = [piece.reshape(-1, lanes) for piece in pieces]
    cuts = np.cumsum([piece.shape[0] for piece in pieces])
    pieces.append(jnp.zeros((-int(cuts[-1]) % 8, lanes), jnp.float32))
    known = lax.all_gather(jnp.concatenate(pieces), "pw", axis=0, tiled=False)

    send, sorted_key = sort_call(rank, key, wave_coeffs, pw_count, size)
    _, pairs = send.shape[1:3]
    blocks_each = local_waves // size
    keys = sorted_key.astype(jnp.float32).reshape(1, -1, pairs, lanes)
    send = send.at[:, blocks_each:].set(jnp.broadcast_to(keys, (pw_count,) + keys.shape[1:]))
    compact = exchange(send)

    spheres, matching_table, phase = sphere_call(
        atom_types, miller, positions, sphere_radii, wave_coeffs, kinds, funcs_each, 2.0 / size
    )
    onehot = (atom_types[:, None] == jnp.arange(kinds, dtype=jnp.int32)[None, :]).astype(
        jnp.float32
    )
    chosen = jnp.einsum("at,tfk->afk", onehot, h_blocks, precision=PRECISE)

    codes, field = prepare_call(known, local_waves, planes_each, size)
    codes = codes.reshape(size * size, lanes)
    field = field.reshape(size * size, lanes)
    offsets = jnp.arange(pw_count, dtype=jnp.int32)[:, None]
    all_starts = known[:, cuts[2] : cuts[3]].reshape(pw_count, lines).astype(jnp.int32)
    all_starts = (all_starts + offsets * local_waves).reshape(-1)
    total = pw_count * local_waves
    ends = jnp.concatenate([all_starts[1:], jnp.full((1,), total, jnp.int32)])
    window = jnp.minimum(all_starts // (size // 2), total // (size // 2) - 1)
    reach = (all_starts % (size // 2)) + (ends - all_starts)
    deep = jnp.max(reach.reshape(size, size), axis=1) > size

    all_keys = compact[:, blocks_each:].astype(jnp.int32).reshape(pw_count, -1)
    all_keys = (all_keys + offsets * (lines * size)).reshape(-1, size)
    slot_row = all_keys // size
    slot_y = all_keys % size
    spheres, slot_y = lax.optimization_barrier((spheres, slot_y))
    spheres = lax.psum(spheres, "pw")
    spheres = spheres.reshape(atom_total, funcs_each, local_bands)
    left, right = interstitial_tables(size)
    back = grid_call(
        window,
        deep.astype(jnp.int32),
        slot_row[:, 0],
        slot_row[:, -1],
        codes,
        jnp.concatenate([slot_row, slot_row], axis=1),
        jnp.concatenate([slot_y, slot_y + size], axis=1),
        field,
        left,
        right,
        compact,
        size,
    )
    back = exchange(back.reshape(pw_count, blocks_each, pairs, lanes))
    applied = jnp.einsum("akb,afk->baf", spheres, chosen, precision=PRECISE)
    muffin = muffin_call(
        atom_types, matching_table, phase, applied.reshape(local_bands, -1), kinetic, wave_coeffs
    )
    h_applied, partial = finish_call(rank, where, back, muffin, columns)
    rows_each = group_count * local_bands // pw_count
    gathered = exchange(partial.reshape(pw_count, rows_each, local_bands))
    return (h_applied, jnp.sum(gathered, axis=0))


def solution(mesh):
    in_specs = (P("pw", "band"), P(None, "pw"), P(), P(), P(), P(), P("pw", None, None))
    out_specs = (P("pw", "band"), P("pw", "band"))
    return jax.shard_map(
        whole_step, mesh=mesh, in_specs=in_specs, out_specs=out_specs, check_vma=False
    )
```

```python
import functools
import math

import jax
import jax.numpy as jnp
import numpy as np
from jax import lax
from jax.experimental import pallas as pl
from jax.experimental.pallas import tpu as pltpu
from jax.sharding import PartitionSpec as P

NPW = 32768


PRECISE = lax.Precision.HIGHEST


def double_factorial(value):
    result = 1
    while value > 1:
        result = result * value
        value = value - 2
    return float(result)


def bessel_table(argument, count):
    safe = jnp.maximum(argument, 1.0)
    upward = [jnp.sin(safe) / safe, jnp.sin(safe) / (safe * safe) - jnp.cos(safe) / safe]
    for degree in range(1, count - 1):
        upward.append((2 * degree + 1) / safe * upward[degree] - upward[degree - 1])
    half_square = -0.5 * argument * argument
    power = jnp.ones_like(argument)
    columns = []
    for degree in range(count):
        term = jnp.ones_like(argument)
        total = jnp.ones_like(argument)
        for index in range(1, 17):
            term = term * half_square / float(index * (2 * degree + 2 * index + 1))
            total = total + term
        series = power * total / double_factorial(2 * degree + 1)
        power = power * argument
        columns.append(jnp.where(argument > degree + 1, upward[degree], series))
    return columns


def harmonic_table(unit, count):
    along_x, along_y, along_z = (unit[0], unit[1], unit[2])
    ones = jnp.ones_like(along_z)
    cosines = [ones]
    sines = [jnp.zeros_like(along_z)]
    for azimuth in range(1, count):
        cosines.append(along_x * cosines[-1] - along_y * sines[-1])
        sines.append(along_x * sines[-2 + 1] + along_y * cosines[-2])
    legendre = {}
    for azimuth in range(count):
        legendre[azimuth, azimuth] = double_factorial(2 * azimuth - 1) * ones
        if azimuth + 1 < count:
            legendre[azimuth + 1, azimuth] = (
                (2 * azimuth + 1) * along_z * legendre[azimuth, azimuth]
            )
        for degree in range(azimuth + 2, count):
            legendre[degree, azimuth] = (
                (2 * degree - 1) * along_z * legendre[degree - 1, azimuth]
                - (degree + azimuth - 1) * legendre[degree - 2, azimuth]
            ) / float(degree - azimuth)
    columns = []
    for degree in range(count):
        for signed in range(-degree, degree + 1):
            azimuth = abs(signed)
            weight = math.sqrt(
                (2 * degree + 1)
                * math.factorial(degree - azimuth)
                / (4.0 * math.pi * math.factorial(degree + azimuth))
            )
            if azimuth > 0:
                weight = weight * math.sqrt(2.0)
            circle = cosines[azimuth] if signed >= 0 else sines[azimuth]
            columns.append(weight * legendre[degree, azimuth] * circle)
    return columns


def cas_matrix(grid_size):
    across = jnp.arange(grid_size, dtype=jnp.int32)
    phase = across[:, None] * across[None, :] % grid_size
    angle = 2.0 * math.pi / grid_size * phase.astype(jnp.float32)
    return (jnp.cos(angle) + jnp.sin(angle)) / math.sqrt(grid_size)


def split_bf16(value):
    high = value.astype(jnp.bfloat16)
    low = (value - high.astype(jnp.float32)).astype(jnp.bfloat16)
    return high, low


def dot32(left, right):
    return jnp.dot(left, right, preferred_element_type=jnp.float32)


def params(*semantics):
    return pltpu.CompilerParams(
        dimension_semantics=semantics or None, vmem_limit_bytes=56 * 1024 * 1024
    )


def fill_matching(types_ref, table_ref, phase_ref, high_ref, low_ref):
    atoms = phase_ref.shape[0]
    funcs = table_ref.shape[1]

    def one(atom, carry):
        tile = table_ref[types_ref[atom]] * phase_ref[pl.ds(atom, 1), :]
        high, low = split_bf16(tile)
        start = pl.multiple_of(atom * funcs, funcs)
        high_ref[pl.ds(start, funcs), :] = high
        low_ref[pl.ds(start, funcs), :] = low
        return carry

    lax.fori_loop(0, atoms, one, 0, unroll=4)


def fill_tables(miller_ref, places_ref, radii_ref, table_ref, phase_ref, angular_ref, spacing):
    kinds, funcs, _ = table_ref.shape
    degree_count = math.isqrt(funcs)
    miller = miller_ref[...].astype(jnp.float32)
    along = [miller[axis : axis + 1, :] for axis in range(3)]
    norm = jnp.sqrt(along[0] * along[0] + along[1] * along[1] + along[2] * along[2])
    scale = jnp.maximum(norm, 1.0)
    for index, column in enumerate(harmonic_table([part / scale for part in along], degree_count)):
        angular_ref[index : index + 1, :] = column
    argument = radii_ref[...] * norm * spacing
    weight = 4.0 * math.pi * NPW ** (-0.5)
    for degree, column in enumerate(bessel_table(argument, degree_count)):
        first, last = degree * degree, (degree + 1) * (degree + 1)
        rows = angular_ref[first:last, :]
        for kind in range(kinds):
            table_ref[kind, first:last, :] = rows * (column[kind : kind + 1, :] * weight)
    places = places_ref[...]
    turns = sum(places[:, axis : axis + 1] * along[axis] for axis in range(3))
    angle = 2.0 * math.pi * (turns - jnp.round(turns))
    phase_ref[...] = jnp.cos(angle) + jnp.sin(angle)


def sphere_kernel(
    types_ref,
    miller_ref,
    places_ref,
    radii_ref,
    wave_ref,
    out_ref,
    table_ref,
    phase_ref,
    angular_ref,
    high_ref,
    low_ref,
    *,
    spacing,
):
    bands = wave_ref.shape[1]

    @pl.when(pl.program_id(0) == 0)
    def _():
        out_ref[...] = jnp.zeros_like(out_ref)

    fill_tables(miller_ref, places_ref, radii_ref, table_ref, phase_ref, angular_ref, spacing)
    fill_matching(types_ref, table_ref, phase_ref, high_ref, low_ref)
    wave_high, wave_low = split_bf16(wave_ref[...])
    both = jnp.concatenate([wave_high, wave_low], axis=1)
    rows = out_ref.shape[0]
    step = math.gcd(rows, 512)
    for first in range(0, rows, step):
        main = dot32(high_ref[first : first + step, :], both)
        rest = dot32(low_ref[first : first + step, :], wave_high)
        out_ref[first : first + step, :] += main[:, :bands] + main[:, bands:] + rest


def sphere_call(types, miller, positions, radii, wave, kinds, funcs, spacing):
    waves, bands = wave.shape
    atoms = positions.shape[1]
    block = math.gcd(waves, 1024)
    rows = atoms * funcs
    return pl.pallas_call(
        functools.partial(sphere_kernel, spacing=spacing),
        grid=(waves // block,),
        in_specs=[
            pl.BlockSpec(memory_space=pltpu.SMEM),
            pl.BlockSpec((3, block), lambda i: (0, i)),
            pl.BlockSpec((atoms, 3), lambda i: (0, 0)),
            pl.BlockSpec((kinds, 1), lambda i: (0, 0)),
            pl.BlockSpec((block, bands), lambda i: (i, 0)),
        ],
        out_specs=[
            pl.BlockSpec((rows, bands), lambda i: (0, 0)),
            pl.BlockSpec((kinds, funcs, block), lambda i: (0, 0, i)),
            pl.BlockSpec((atoms, block), lambda i: (0, i)),
        ],
        out_shape=[
            jax.ShapeDtypeStruct((rows, bands), jnp.float32),
            jax.ShapeDtypeStruct((kinds, funcs, waves), jnp.float32),
            jax.ShapeDtypeStruct((atoms, waves), jnp.float32),
        ],
        scratch_shapes=[
            pltpu.VMEM((funcs, block), jnp.float32),
            pltpu.VMEM((rows, block), jnp.bfloat16),
            pltpu.VMEM((rows, block), jnp.bfloat16),
        ],
        compiler_params=params("arbitrary"),
        cost_estimate=pl.CostEstimate(
            flops=6 * waves * rows * bands, bytes_accessed=8 * waves * bands, transcendentals=0
        ),
        name="sphere",
    )(types, miller, positions.T, radii[:, None], wave)


def muffin_kernel(
    types_ref,
    table_ref,
    phase_ref,
    sphere_ref,
    kinetic_ref,
    wave_ref,
    out_ref,
    high_ref,
    low_ref,
):
    bands = out_ref.shape[0]
    fill_matching(types_ref, table_ref, phase_ref, high_ref, low_ref)
    high, low = split_bf16(sphere_ref[...])
    main = dot32(jnp.concatenate([high, low], axis=0), high_ref[...])
    rest = dot32(high, low_ref[...])
    kinetic = kinetic_ref[...] * wave_ref[...].T
    out_ref[...] = main[:bands, :] + main[bands:, :] + rest + kinetic


def muffin_call(types, table, phase, sphere, kinetic, wave):
    kinds, funcs, waves = table.shape
    atoms = phase.shape[0]
    bands, rows = sphere.shape
    block = math.gcd(waves, 1024)
    return pl.pallas_call(
        muffin_kernel,
        grid=(waves // block,),
        in_specs=[
            pl.BlockSpec(memory_space=pltpu.SMEM),
            pl.BlockSpec((kinds, funcs, block), lambda i: (0, 0, i)),
            pl.BlockSpec((atoms, block), lambda i: (0, i)),
            pl.BlockSpec((bands, rows), lambda i: (0, 0)),
            pl.BlockSpec((1, block), lambda i: (0, i)),
            pl.BlockSpec((block, bands), lambda i: (i, 0)),
        ],
        out_specs=pl.BlockSpec((bands, block), lambda i: (0, i)),
        out_shape=jax.ShapeDtypeStruct((bands, waves), jnp.float32),
        scratch_shapes=[
            pltpu.VMEM((rows, block), jnp.bfloat16),
            pltpu.VMEM((rows, block), jnp.bfloat16),
        ],
        compiler_params=params("arbitrary"),
        cost_estimate=pl.CostEstimate(
            flops=6 * waves * rows * bands, bytes_accessed=8 * waves * bands, transcendentals=0
        ),
        name="muffin",
    )(types, table, phase, sphere, kinetic[None, :], wave)


def sort_kernel(rank_ref, key_ref, wave_ref, send_ref, sorted_ref, rows_ref):
    waves, _ = wave_ref.shape
    parts, _, pairs, lanes = send_ref.shape
    half = lanes // 2

    def place(index, carry):
        target = rank_ref[index]
        rows_ref[pl.ds(target, 1), :] = wave_ref[pl.ds(index, 1), :]
        sorted_ref[target] = key_ref[index]
        return carry

    lax.fori_loop(0, waves, place, 0, unroll=32)

    def turn(tile, carry):
        start = pl.multiple_of(tile * lanes, lanes)
        turned = rows_ref[pl.ds(start, lanes), :].T
        for part in range(parts):
            first = part * 2 * pairs
            top = turned[first : first + pairs, :]
            low = turned[first + pairs : first + 2 * pairs, :]
            send_ref[part, 2 * tile] = jnp.concatenate([top[:, :half], low[:, :half]], axis=1)
            send_ref[part, 2 * tile + 1] = jnp.concatenate([top[:, half:], low[:, half:]], axis=1)
        return carry

    lax.fori_loop(0, waves // lanes, turn, 0, unroll=4)


def sort_call(rank, key, wave, parts, half):
    waves, bands = wave.shape
    pairs = bands // parts // 2
    stored = waves // half + waves // (pairs * 2 * half)
    return pl.pallas_call(
        sort_kernel,
        in_specs=[
            pl.BlockSpec(memory_space=pltpu.SMEM),
            pl.BlockSpec(memory_space=pltpu.SMEM),
            pl.BlockSpec(memory_space=pltpu.VMEM),
        ],
        out_specs=[
            pl.BlockSpec(memory_space=pltpu.VMEM),
            pl.BlockSpec(memory_space=pltpu.SMEM),
        ],
        out_shape=[
            jax.ShapeDtypeStruct((parts, stored, pairs, 2 * half), jnp.float32),
            jax.ShapeDtypeStruct((waves,), jnp.int32),
        ],
        scratch_shapes=[pltpu.VMEM((waves, bands), jnp.float32)],
        compiler_params=params(),
        name="sort",
    )(rank, key, wave)


def lane_gather(values, index):
    numbers = lax.GatherDimensionNumbers(
        offset_dims=(),
        collapsed_slice_dims=(1,),
        start_index_map=(1,),
        operand_batching_dims=(0,),
        start_indices_batching_dims=(0,),
    )
    return lax.gather(
        values,
        index[..., None],
        numbers,
        slice_sizes=(1, 1),
        mode=lax.GatherScatterMode.PROMISE_IN_BOUNDS,
    )


def grid_kernel(
    window_ref,
    deep_ref,
    first_ref,
    last_ref,
    code_ref,
    slot_row_ref,
    slot_y_ref,
    potential_ref,
    left_ref,
    right_ref,
    compact_ref,
    out_ref,
    grid_ref,
    windows_ref,
    *,
    size,
    pitch,
    band_pitch,
    wide,
):
    blocks, pairs, lanes = out_ref.shape
    half = lanes // 2
    rows = size * size
    shift = size.bit_length() - 1
    extra = pitch - size
    upper = lax.broadcasted_iota(jnp.int32, (pairs, lanes), 1) // half * half
    parts, _, _, _ = compact_ref.shape
    each = blocks // parts
    inner = lax.broadcasted_iota(jnp.int32, (pairs, lanes), 1) % half
    steps = math.gcd(each, 16)

    def widen(part, carry):
        following = jnp.minimum(part + 1, parts - 1)

        def some(group, carry):
            first = group * steps
            for step in range(steps):
                block = compact_ref[part, first + step]
                if step + 1 < steps:
                    after = compact_ref[part, first + step + 1]
                else:
                    inside = first + steps < each
                    after = compact_ref[
                        jnp.where(inside, part, following), jnp.where(inside, first + steps, 0)
                    ]
                mixed = jnp.where(
                    inner < half // 2,
                    pltpu.roll(block, lanes - half // 2, 1),
                    pltpu.roll(after, half // 2, 1),
                )
                spot = 2 * (part * each + first + step)
                windows_ref[spot] = block
                windows_ref[spot + 1] = mixed
            return carry

        return lax.fori_loop(0, each // steps, some, carry)

    lax.fori_loop(0, parts, widen, 0)

    def expand(group, carry):
        base = group * wide
        place = base + lax.shift_right_logical(base, shift) * extra

        @pl.when(deep_ref[group] == 0)
        def _():
            for step in range(wide):
                row = base + step
                code = jnp.broadcast_to(code_ref[pl.ds(row, 1), :], (pairs, lanes))
                index = (code & (half - 1)) | upper
                value = lane_gather(windows_ref[window_ref[row]], index)
                value = jnp.where(code >= 0, value, 0.0)
                grid_ref[pl.ds(place + step, pairs, stride=band_pitch), :] = value

        @pl.when(deep_ref[group] != 0)
        def _():
            def one(step, carry):
                row = base + step
                code = jnp.broadcast_to(code_ref[pl.ds(row, 1), :], (pairs, lanes))
                index = (code & (half - 1)) | upper
                window = window_ref[row]
                later = jnp.minimum(window + 2, 2 * blocks - 1)
                here = lane_gather(windows_ref[window], index)
                there = lane_gather(windows_ref[later], index)
                value = jnp.where(code < half, here, there)
                value = jnp.where(code >= 0, value, 0.0)
                grid_ref[pl.ds(place + step, pairs, stride=band_pitch), :] = value
                return carry

            lax.fori_loop(0, wide, one, 0)

        return carry

    lax.fori_loop(0, rows // wide, expand, 0)

    left = left_ref[...]
    right = right_ref[...]

    def apply_left(value):
        high, low = split_bf16(value)
        both = dot32(left, jnp.concatenate([high, low], axis=0))
        return both[:size, :] + both[size:, :]

    def apply_right(value):
        high, low = split_bf16(value)
        both = dot32(jnp.concatenate([high, low], axis=1), right)
        return both[:, :lanes] + both[:, lanes:]

    many = math.gcd(size, 16)

    chains = max(1, math.gcd(size // many, 4))
    groups = size // (many * chains)

    def planes(turn, carry):
        base = turn // groups * band_pitch
        offset = turn % groups * (many * chains * pitch)
        for chain in range(chains):
            starts = [
                pl.multiple_of(base + offset + (chain * many + index) * pitch, 8)
                for index in range(many)
            ]
            field = jnp.concatenate([grid_ref[pl.ds(s, size), :] for s in starts], axis=1)
            field = apply_left(field)
            field = jnp.concatenate(
                [field[:, index * lanes : (index + 1) * lanes] for index in range(many)], axis=0
            )
            field = apply_right(field)
            for index, s in enumerate(starts):
                grid_ref[pl.ds(s, size), :] = field[index * size : (index + 1) * size, :]
        return carry

    def columns(turn, carry):
        along = turn % groups * (many * chains)
        base = turn // groups * band_pitch + along
        for chain in range(chains):
            spots = [chain * many + index for index in range(many)]
            field = jnp.concatenate(
                [grid_ref[pl.ds(base + spot, size, stride=pitch), :] for spot in spots], axis=1
            )
            field = apply_left(field)
            weight = jnp.concatenate(
                [
                    potential_ref[pl.ds(pl.multiple_of((along + spot) * size, size), size), :]
                    for spot in spots
                ],
                axis=1,
            )
            field = apply_left(field * weight)
            for index, spot in enumerate(spots):
                grid_ref[pl.ds(base + spot, size, stride=pitch), :] = field[
                    :, index * lanes : (index + 1) * lanes
                ]
        return carry

    turns = pairs * groups
    lax.fori_loop(0, turns, planes, 0)
    lax.fori_loop(0, turns, columns, 0)
    lax.fori_loop(0, turns, planes, 0)

    visits = 12

    def visit(row, wanted, index, value):
        source = row + lax.shift_right_logical(row, shift) * extra
        here = lane_gather(grid_ref[pl.ds(source, pairs, stride=band_pitch), :], index)
        return jnp.where(wanted == row, here, value)

    def slots(block):
        wanted = jnp.broadcast_to(slot_row_ref[pl.ds(block, 1), :], (pairs, lanes))
        index = jnp.broadcast_to(slot_y_ref[pl.ds(block, 1), :], (pairs, lanes))
        return wanted, index

    together = math.gcd(blocks, 16)

    def collect(group, carry):
        longest = 0
        for step in range(together):
            block = group * together + step
            wanted, index = slots(block)
            first = first_ref[block]
            value = jnp.zeros((pairs, lanes), jnp.float32)
            for number in range(visits):
                value = visit(first + number, wanted, index, value)
            out_ref[block] = value
            longest = jnp.maximum(longest, last_ref[block] - first)

        @pl.when(longest >= visits)
        def _():
            for step in range(together):
                block = group * together + step
                wanted, index = slots(block)
                first = first_ref[block]
                out_ref[block] = lax.fori_loop(
                    first + visits,
                    last_ref[block] + 1,
                    lambda row, value: visit(row, wanted, index, value),
                    out_ref[block],
                )

        return carry

    lax.fori_loop(0, blocks // together, collect, 0)


def grid_call(window, deep, first, last, code, slot_row, slot_y, field, left, right, compact, size):
    _, _, pairs, lanes = compact.shape
    blocks = first.shape[0]
    pitch = size + 8
    band_pitch = size * pitch + 8
    smem = pl.BlockSpec(memory_space=pltpu.SMEM)
    vmem = pl.BlockSpec(memory_space=pltpu.VMEM)
    points = 2 * pairs * size**3
    return pl.pallas_call(
        functools.partial(
            grid_kernel,
            size=size,
            pitch=pitch,
            band_pitch=band_pitch,
            wide=size * size // deep.shape[0],
        ),
        in_specs=[smem] * 4 + [vmem] * 7,
        out_specs=vmem,
        out_shape=jax.ShapeDtypeStruct((blocks, pairs, lanes), jnp.float32),
        scratch_shapes=[
            pltpu.VMEM((pairs * band_pitch + 16, lanes), jnp.float32),
            pltpu.VMEM((2 * blocks, pairs, lanes), jnp.float32),
        ],
        compiler_params=params(),
        cost_estimate=pl.CostEstimate(
            flops=36 * size * points, bytes_accessed=4 * points, transcendentals=0
        ),
        name="grid",
    )(window, deep, first, last, code, slot_row, slot_y, field, left, right, compact)


def prepare_kernel(known_ref, lanes_ref, rows_ref, code_ref, field_ref, *, waves, low_count, size):
    lanes = known_ref.shape[2]
    left_ids, right_ids = rows_ref.shape[0], lanes_ref.shape[0]
    field_rows = code_ref.shape[1] // 2
    wave_rows = waves // lanes
    part = pl.program_id(0)

    def onehot(first, count):
        ids = lax.broadcasted_iota(jnp.int32, (count, lanes), 0).astype(jnp.float32)
        return jnp.concatenate(
            [
                jnp.where(known_ref[0, row : row + 1, :] == ids, 1.0, 0.0).astype(jnp.bfloat16)
                for row in range(first, first + wave_rows)
            ],
            axis=1,
        )

    filled = lax.dot_general(
        onehot(field_rows, left_ids),
        onehot(field_rows + wave_rows, right_ids),
        (((1,), (1,)), ((), ())),
        preferred_element_type=jnp.float32,
    )
    sums = dot32(filled.astype(jnp.bfloat16), lanes_ref[...])
    ahead = sums[:, :right_ids]
    counts = jnp.concatenate(
        [sums[:, index * right_ids : (index + 1) * right_ids] for index in (1, 2, 3)], axis=0
    )
    start = dot32(rows_ref[...], counts.astype(jnp.bfloat16)).astype(jnp.int32) + part * waves
    code = ahead.astype(jnp.int32) + (start & (size // 2 - 1))
    code = jnp.where(filled > 0.5, code, -1)
    for low in range(low_count):
        piece = code[:, low * size : (low + 1) * size]
        piece = jnp.concatenate([piece, piece], axis=1)
        for high in range(left_ids // size):
            first = (high * low_count + low) * size
            code_ref[0, first : first + size, :] = piece[high * size : (high + 1) * size, :]
    field = known_ref[0, :field_rows, :]
    for side in range(2):
        half = field[:, side * size : (side + 1) * size]
        field_ref[0, pl.ds(side, field_rows, stride=2), :] = jnp.concatenate([half, half], axis=1)


def prepare_call(known, waves, planes_each, size):
    parts, stored, lanes = known.shape
    low_count = math.gcd(planes_each, 4)
    high_count = planes_each // low_count
    lines = planes_each * size
    eye = np.eye(low_count)
    square = np.ones((size, size))
    before = np.triu(square, 1)
    lanes_table = np.concatenate(
        [
            np.kron(eye, before),
            np.kron(eye, square),
            np.kron(np.triu(np.ones((low_count, low_count)), 1), square),
            np.kron(np.ones((low_count, low_count)), square),
        ],
        axis=1,
    )
    eye = np.eye(high_count)
    rows_table = np.concatenate(
        [
            np.kron(eye, before.T),
            np.kron(eye, square),
            np.kron(np.tril(np.ones((high_count, high_count)), -1), square),
        ],
        axis=1,
    )
    return pl.pallas_call(
        functools.partial(prepare_kernel, waves=waves, low_count=low_count, size=size),
        grid=(parts,),
        in_specs=[
            pl.BlockSpec((1, stored, lanes), lambda i: (i, 0, 0)),
            pl.BlockSpec(lanes_table.shape, lambda i: (0, 0)),
            pl.BlockSpec(rows_table.shape, lambda i: (0, 0)),
        ],
        out_specs=[pl.BlockSpec((1, lines, lanes), lambda i: (i, 0, 0))] * 2,
        out_shape=[
            jax.ShapeDtypeStruct((parts, lines, lanes), jnp.int32),
            jax.ShapeDtypeStruct((parts, lines, lanes), jnp.float32),
        ],
        compiler_params=params("arbitrary"),
        cost_estimate=pl.CostEstimate(
            flops=2 * parts * waves * lines * size, bytes_accessed=4 * parts * waves, transcendentals=0
        ),
        name="prepare",
    )(known, jnp.asarray(lanes_table, jnp.bfloat16), jnp.asarray(rows_table, jnp.bfloat16))


def finish_kernel(rank_ref, where_ref, back_ref, muffin_ref, *refs):
    *all_refs, out_ref, sub_ref, rows_ref = refs
    block, bands = out_ref.shape
    parts, _, _, lanes = back_ref.shape
    half = lanes // 2
    turn = pl.program_id(0)

    @pl.when(turn == 0)
    def _():
        sub_ref[...] = jnp.zeros_like(sub_ref)

        def order(tile, carry):
            start = pl.multiple_of(tile * lanes, lanes)
            pieces = []
            for part in range(parts):
                even = back_ref[part, 2 * tile]
                odd = back_ref[part, 2 * tile + 1]
                pieces.append(jnp.concatenate([even[:, :half], odd[:, :half]], axis=1))
                pieces.append(jnp.concatenate([even[:, half:], odd[:, half:]], axis=1))
            rows_ref[pl.ds(start, lanes), :] = jnp.concatenate(pieces, axis=0).T
            return carry

        lax.fori_loop(0, rows_ref.shape[0] // lanes, order, 0, unroll=4)

    first = turn * block

    def place(index, carry):
        out_ref[pl.ds(index, 1), :] = rows_ref[pl.ds(rank_ref[first + index], 1), :]
        return carry

    lax.fori_loop(0, block, place, 0, unroll=64)
    applied = muffin_ref[...] + out_ref[...].T
    out_ref[...] = applied.T
    high, low = split_bf16(applied)
    both = jnp.concatenate([high, low], axis=0)
    for shift, all_ref in enumerate(all_refs):
        all_high, all_low = split_bf16(all_ref[...])
        main = dot32(both, all_high)
        total = main[:bands, :] + main[bands:, :] + dot32(high, all_low)
        sub_ref[where_ref[shift]] += total

    @pl.when(turn == pl.num_programs(0) - 1)
    def _():
        for group in range(sub_ref.shape[0]):
            sub_ref[group] = sub_ref[group].T * NPW ** (-0.5)


def finish_call(rank, where, back, muffin, columns):
    bands, waves = muffin.shape
    groups = len(columns)
    block = math.gcd(waves, 2048)
    return pl.pallas_call(
        finish_kernel,
        grid=(waves // block,),
        in_specs=[
            pl.BlockSpec(memory_space=pltpu.SMEM),
            pl.BlockSpec(memory_space=pltpu.SMEM),
            pl.BlockSpec(back.shape, lambda i: (0, 0, 0, 0)),
            pl.BlockSpec((bands, block), lambda i: (0, i)),
        ]
        + [pl.BlockSpec((block, bands), lambda i: (i, 0))] * groups,
        out_specs=[
            pl.BlockSpec((block, bands), lambda i: (i, 0)),
            pl.BlockSpec((groups, bands, bands), lambda i: (0, 0, 0)),
        ],
        out_shape=[
            jax.ShapeDtypeStruct((waves, bands), jnp.float32),
            jax.ShapeDtypeStruct((groups, bands, bands), jnp.float32),
        ],
        scratch_shapes=[pltpu.VMEM((waves, bands), jnp.float32)],
        compiler_params=params("arbitrary"),
        name="finish",
    )(rank, where, back, muffin, *columns)


def exchange(array):
    return lax.all_to_all(array, "pw", split_axis=0, concat_axis=0, tiled=True)


def round_high(value):
    return lax.reduce_precision(value, 8, 7)


def interstitial_tables(size):
    table = cas_matrix(size)
    high = round_high(table)
    low = round_high(table - high)
    zero = jnp.zeros_like(table)
    left = jnp.concatenate(
        [jnp.concatenate([high, high], axis=1), jnp.concatenate([low, zero], axis=1)], axis=0
    )

    def twice(block):
        return jnp.concatenate(
            [jnp.concatenate([block, zero], axis=1), jnp.concatenate([zero, block], axis=1)], axis=0
        )

    right = jnp.concatenate(
        [
            jnp.concatenate([twice(high), twice(low)], axis=1),
            jnp.concatenate([twice(high), jnp.zeros((2 * size, 2 * size))], axis=1),
        ],
        axis=0,
    )
    return left.astype(jnp.bfloat16), right.astype(jnp.bfloat16)


def whole_step(wave_coeffs, miller, atom_types, positions, sphere_radii, h_blocks, potential):
    pw_count = lax.axis_size("pw")
    pw_index = lax.axis_index("pw")
    local_waves, local_bands = wave_coeffs.shape
    size = potential.shape[1]
    kinds, funcs_each = h_blocks.shape[:2]
    atom_total = atom_types.shape[0]
    miller_float = miller.astype(jnp.float32)
    kinetic = jnp.sum(miller_float * miller_float, axis=0) / 1536.0
    planes_each = size // pw_count
    lines = planes_each * size

    group_count = lax.axis_size("band")
    group = lax.axis_index("band")
    columns = [wave_coeffs]
    for shift in range(1, group_count):
        route = [(index, (index + shift) % group_count) for index in range(group_count)]
        columns.append(lax.ppermute(wave_coeffs, "band", route))
    where = jnp.mod(group - jnp.arange(group_count, dtype=jnp.int32), group_count)

    wrapped = jnp.mod(miller, size)
    line = (wrapped[2] - pw_index * planes_each) * size + wrapped[0]
    key = line * size + wrapped[1]
    rank = jnp.sum((key[:, None] < key[None, :]).astype(jnp.int32), axis=0)
    lanes = 2 * size
    low_count = math.gcd(planes_each, 4)
    plane = wrapped[2] - pw_index * planes_each
    starts = jnp.sum(
        (line[:, None] < jnp.arange(lines, dtype=jnp.int32)[None, :]).astype(jnp.int32), axis=0
    )
    pieces = [
        jnp.transpose(potential, (0, 2, 1)),
        (plane // low_count * size + wrapped[0]).astype(jnp.float32),
        (plane % low_count * size + wrapped[1]).astype(jnp.float32),
        starts.astype(jnp.float32),
    ]
    pieces = [piece.reshape(-1, lanes) for piece in pieces]
    cuts = np.cumsum([piece.shape[0] for piece in pieces])
    pieces.append(jnp.zeros((-int(cuts[-1]) % 8, lanes), jnp.float32))
    known = jnp.concatenate(pieces)
    known = exchange(jnp.broadcast_to(known[None], (pw_count,) + known.shape))

    send, sorted_key = sort_call(rank, key, wave_coeffs, pw_count, size)
    _, pairs = send.shape[1:3]
    blocks_each = local_waves // size
    keys = sorted_key.astype(jnp.float32).reshape(1, -1, pairs, lanes)
    send = send.at[:, blocks_each:].set(jnp.broadcast_to(keys, (pw_count,) + keys.shape[1:]))
    compact = exchange(send)

    spheres, matching_table, phase = sphere_call(
        atom_types, miller, positions, sphere_radii, wave_coeffs, kinds, funcs_each, 2.0 / size
    )
    onehot = (atom_types[:, None] == jnp.arange(kinds, dtype=jnp.int32)[None, :]).astype(
        jnp.float32
    )
    chosen = jnp.einsum("at,tfk->afk", onehot, h_blocks, precision=PRECISE)

    codes, field = prepare_call(known, local_waves, planes_each, size)
    codes = codes.reshape(size * size, lanes)
    field = field.reshape(size * size, lanes)
    offsets = jnp.arange(pw_count, dtype=jnp.int32)[:, None]
    all_starts = known[:, cuts[2] : cuts[3]].reshape(pw_count, lines).astype(jnp.int32)
    all_starts = (all_starts + offsets * local_waves).reshape(-1)
    total = pw_count * local_waves
    ends = jnp.concatenate([all_starts[1:], jnp.full((1,), total, jnp.int32)])
    window = jnp.minimum(all_starts // (size // 2), total // (size // 2) - 1)
    reach = (all_starts % (size // 2)) + (ends - all_starts)
    deep = jnp.max(reach.reshape(size, size), axis=1) > size

    all_keys = compact[:, blocks_each:].astype(jnp.int32).reshape(pw_count, -1)
    all_keys = (all_keys + offsets * (lines * size)).reshape(-1, size)
    slot_row = all_keys // size
    slot_y = all_keys % size
    spheres, slot_y = lax.optimization_barrier((spheres, slot_y))
    spheres = lax.psum(spheres, "pw")
    spheres = spheres.reshape(atom_total, funcs_each, local_bands)
    left, right = interstitial_tables(size)
    back = grid_call(
        window,
        deep.astype(jnp.int32),
        slot_row[:, 0],
        slot_row[:, -1],
        codes,
        jnp.concatenate([slot_row, slot_row], axis=1),
        jnp.concatenate([slot_y, slot_y + size], axis=1),
        field,
        left,
        right,
        compact,
        size,
    )
    back = exchange(back.reshape(pw_count, blocks_each, pairs, lanes))
    applied = jnp.einsum("akb,afk->baf", spheres, chosen, precision=PRECISE)
    muffin = muffin_call(
        atom_types, matching_table, phase, applied.reshape(local_bands, -1), kinetic, wave_coeffs
    )
    h_applied, partial = finish_call(rank, where, back, muffin, columns)
    rows_each = group_count * local_bands // pw_count
    gathered = exchange(partial.reshape(pw_count, rows_each, local_bands))
    return (h_applied, jnp.sum(gathered, axis=0))


def solution(mesh):
    in_specs = (P("pw", "band"), P(None, "pw"), P(), P(), P(), P(), P("pw", None, None))
    out_specs = (P("pw", "band"), P("pw", "band"))
    return jax.shard_map(
        whole_step, mesh=mesh, in_specs=in_specs, out_specs=out_specs, check_vma=False
    )
```

```python
import functools
import math

import jax
import jax.numpy as jnp
import numpy as np
from jax import lax
from jax.experimental import pallas as pl
from jax.experimental.pallas import tpu as pltpu
from jax.sharding import PartitionSpec as P

NPW = 32768


PRECISE = lax.Precision.HIGHEST


def double_factorial(value):
    result = 1
    while value > 1:
        result = result * value
        value = value - 2
    return float(result)


def bessel_table(argument, count):
    safe = jnp.maximum(argument, 1.0)
    upward = [jnp.sin(safe) / safe, jnp.sin(safe) / (safe * safe) - jnp.cos(safe) / safe]
    for degree in range(1, count - 1):
        upward.append((2 * degree + 1) / safe * upward[degree] - upward[degree - 1])
    half_square = -0.5 * argument * argument
    power = jnp.ones_like(argument)
    columns = []
    for degree in range(count):
        term = jnp.ones_like(argument)
        total = jnp.ones_like(argument)
        for index in range(1, 17):
            term = term * half_square / float(index * (2 * degree + 2 * index + 1))
            total = total + term
        series = power * total / double_factorial(2 * degree + 1)
        power = power * argument
        columns.append(jnp.where(argument > degree + 1, upward[degree], series))
    return columns


def harmonic_table(unit, count):
    along_x, along_y, along_z = (unit[0], unit[1], unit[2])
    ones = jnp.ones_like(along_z)
    cosines = [ones]
    sines = [jnp.zeros_like(along_z)]
    for azimuth in range(1, count):
        cosines.append(along_x * cosines[-1] - along_y * sines[-1])
        sines.append(along_x * sines[-2 + 1] + along_y * cosines[-2])
    legendre = {}
    for azimuth in range(count):
        legendre[azimuth, azimuth] = double_factorial(2 * azimuth - 1) * ones
        if azimuth + 1 < count:
            legendre[azimuth + 1, azimuth] = (
                (2 * azimuth + 1) * along_z * legendre[azimuth, azimuth]
            )
        for degree in range(azimuth + 2, count):
            legendre[degree, azimuth] = (
                (2 * degree - 1) * along_z * legendre[degree - 1, azimuth]
                - (degree + azimuth - 1) * legendre[degree - 2, azimuth]
            ) / float(degree - azimuth)
    columns = []
    for degree in range(count):
        for signed in range(-degree, degree + 1):
            azimuth = abs(signed)
            weight = math.sqrt(
                (2 * degree + 1)
                * math.factorial(degree - azimuth)
                / (4.0 * math.pi * math.factorial(degree + azimuth))
            )
            if azimuth > 0:
                weight = weight * math.sqrt(2.0)
            circle = cosines[azimuth] if signed >= 0 else sines[azimuth]
            columns.append(weight * legendre[degree, azimuth] * circle)
    return columns


def split_bf16(value):
    high = value.astype(jnp.bfloat16)
    low = (value - high.astype(jnp.float32)).astype(jnp.bfloat16)
    return high, low


def dot32(left, right):
    return jnp.dot(left, right, preferred_element_type=jnp.float32)


def params(*semantics):
    return pltpu.CompilerParams(
        dimension_semantics=semantics or None, vmem_limit_bytes=56 * 1024 * 1024
    )


def fill_matching(types_ref, table_ref, phase_ref, high_ref, low_ref):
    atoms = phase_ref.shape[0]
    funcs = table_ref.shape[1]

    def one(atom, carry):
        tile = table_ref[types_ref[atom]] * phase_ref[pl.ds(atom, 1), :]
        high, low = split_bf16(tile)
        start = pl.multiple_of(atom * funcs, funcs)
        high_ref[pl.ds(start, funcs), :] = high
        low_ref[pl.ds(start, funcs), :] = low
        return carry

    lax.fori_loop(0, atoms, one, 0, unroll=4)


def fill_tables(miller_ref, places_ref, radii_ref, table_ref, phase_ref, angular_ref, spacing):
    kinds, funcs, _ = table_ref.shape
    degree_count = math.isqrt(funcs)
    miller = miller_ref[...].astype(jnp.float32)
    along = [miller[axis : axis + 1, :] for axis in range(3)]
    norm = jnp.sqrt(along[0] * along[0] + along[1] * along[1] + along[2] * along[2])
    scale = jnp.maximum(norm, 1.0)
    for index, column in enumerate(harmonic_table([part / scale for part in along], degree_count)):
        angular_ref[index : index + 1, :] = column
    argument = radii_ref[...] * norm * spacing
    weight = 4.0 * math.pi * NPW ** (-0.5)
    for degree, column in enumerate(bessel_table(argument, degree_count)):
        first, last = degree * degree, (degree + 1) * (degree + 1)
        rows = angular_ref[first:last, :]
        for kind in range(kinds):
            table_ref[kind, first:last, :] = rows * (column[kind : kind + 1, :] * weight)
    places = places_ref[...]
    turns = sum(places[:, axis : axis + 1] * along[axis] for axis in range(3))
    angle = 2.0 * math.pi * (turns - jnp.round(turns))
    phase_ref[...] = jnp.cos(angle) + jnp.sin(angle)


def sphere_kernel(
    types_ref,
    miller_ref,
    places_ref,
    radii_ref,
    wave_ref,
    out_ref,
    table_ref,
    phase_ref,
    angular_ref,
    high_ref,
    low_ref,
    *,
    spacing,
):
    bands = wave_ref.shape[1]

    @pl.when(pl.program_id(0) == 0)
    def _():
        out_ref[...] = jnp.zeros_like(out_ref)

    fill_tables(miller_ref, places_ref, radii_ref, table_ref, phase_ref, angular_ref, spacing)
    fill_matching(types_ref, table_ref, phase_ref, high_ref, low_ref)
    wave_high, wave_low = split_bf16(wave_ref[...])
    both = jnp.concatenate([wave_high, wave_low], axis=1)
    rows = out_ref.shape[0]
    step = math.gcd(rows, 512)
    for first in range(0, rows, step):
        main = dot32(high_ref[first : first + step, :], both)
        rest = dot32(low_ref[first : first + step, :], wave_high)
        out_ref[first : first + step, :] += main[:, :bands] + main[:, bands:] + rest


def sphere_call(types, miller, positions, radii, wave, kinds, funcs, spacing):
    waves, bands = wave.shape
    atoms = positions.shape[1]
    block = math.gcd(waves, 1024)
    rows = atoms * funcs
    return pl.pallas_call(
        functools.partial(sphere_kernel, spacing=spacing),
        grid=(waves // block,),
        in_specs=[
            pl.BlockSpec(memory_space=pltpu.SMEM),
            pl.BlockSpec((3, block), lambda i: (0, i)),
            pl.BlockSpec((atoms, 3), lambda i: (0, 0)),
            pl.BlockSpec((kinds, 1), lambda i: (0, 0)),
            pl.BlockSpec((block, bands), lambda i: (i, 0)),
        ],
        out_specs=[
            pl.BlockSpec((rows, bands), lambda i: (0, 0)),
            pl.BlockSpec((kinds, funcs, block), lambda i: (0, 0, i)),
            pl.BlockSpec((atoms, block), lambda i: (0, i)),
        ],
        out_shape=[
            jax.ShapeDtypeStruct((rows, bands), jnp.float32),
            jax.ShapeDtypeStruct((kinds, funcs, waves), jnp.float32),
            jax.ShapeDtypeStruct((atoms, waves), jnp.float32),
        ],
        scratch_shapes=[
            pltpu.VMEM((funcs, block), jnp.float32),
            pltpu.VMEM((rows, block), jnp.bfloat16),
            pltpu.VMEM((rows, block), jnp.bfloat16),
        ],
        compiler_params=params("arbitrary"),
        cost_estimate=pl.CostEstimate(
            flops=6 * waves * rows * bands, bytes_accessed=8 * waves * bands, transcendentals=0
        ),
        name="sphere",
    )(types, miller, positions.T, radii[:, None], wave)


def muffin_kernel(
    types_ref,
    table_ref,
    phase_ref,
    sphere_ref,
    kinetic_ref,
    wave_ref,
    out_ref,
    high_ref,
    low_ref,
):
    bands = out_ref.shape[0]
    fill_matching(types_ref, table_ref, phase_ref, high_ref, low_ref)
    high, low = split_bf16(sphere_ref[...])
    main = dot32(jnp.concatenate([high, low], axis=0), high_ref[...])
    rest = dot32(high, low_ref[...])
    kinetic = kinetic_ref[...] * wave_ref[...].T
    out_ref[...] = main[:bands, :] + main[bands:, :] + rest + kinetic


def muffin_call(types, table, phase, sphere, kinetic, wave):
    kinds, funcs, waves = table.shape
    atoms = phase.shape[0]
    bands, rows = sphere.shape
    block = math.gcd(waves, 1024)
    return pl.pallas_call(
        muffin_kernel,
        grid=(waves // block,),
        in_specs=[
            pl.BlockSpec(memory_space=pltpu.SMEM),
            pl.BlockSpec((kinds, funcs, block), lambda i: (0, 0, i)),
            pl.BlockSpec((atoms, block), lambda i: (0, i)),
            pl.BlockSpec((bands, rows), lambda i: (0, 0)),
            pl.BlockSpec((1, block), lambda i: (0, i)),
            pl.BlockSpec((block, bands), lambda i: (i, 0)),
        ],
        out_specs=pl.BlockSpec((bands, block), lambda i: (0, i)),
        out_shape=jax.ShapeDtypeStruct((bands, waves), jnp.float32),
        scratch_shapes=[
            pltpu.VMEM((rows, block), jnp.bfloat16),
            pltpu.VMEM((rows, block), jnp.bfloat16),
        ],
        compiler_params=params("arbitrary"),
        cost_estimate=pl.CostEstimate(
            flops=6 * waves * rows * bands, bytes_accessed=8 * waves * bands, transcendentals=0
        ),
        name="muffin",
    )(types, table, phase, sphere, kinetic[None, :], wave)


def sort_kernel(rank_ref, key_ref, wave_ref, send_ref, sorted_ref, rows_ref):
    waves, _ = wave_ref.shape
    parts, _, pairs, lanes = send_ref.shape
    half = lanes // 2

    def place(index, carry):
        target = rank_ref[index]
        rows_ref[pl.ds(target, 1), :] = wave_ref[pl.ds(index, 1), :]
        sorted_ref[target] = key_ref[index]
        return carry

    lax.fori_loop(0, waves, place, 0, unroll=32)

    def turn(tile, carry):
        start = pl.multiple_of(tile * lanes, lanes)
        turned = rows_ref[pl.ds(start, lanes), :].T
        for part in range(parts):
            first = part * 2 * pairs
            top = turned[first : first + pairs, :]
            low = turned[first + pairs : first + 2 * pairs, :]
            send_ref[part, 2 * tile] = jnp.concatenate([top[:, :half], low[:, :half]], axis=1)
            send_ref[part, 2 * tile + 1] = jnp.concatenate([top[:, half:], low[:, half:]], axis=1)
        return carry

    lax.fori_loop(0, waves // lanes, turn, 0, unroll=4)


def sort_call(rank, key, wave, parts, half):
    waves, bands = wave.shape
    pairs = bands // parts // 2
    stored = waves // half + waves // (pairs * 2 * half)
    return pl.pallas_call(
        sort_kernel,
        in_specs=[
            pl.BlockSpec(memory_space=pltpu.SMEM),
            pl.BlockSpec(memory_space=pltpu.SMEM),
            pl.BlockSpec(memory_space=pltpu.VMEM),
        ],
        out_specs=[
            pl.BlockSpec(memory_space=pltpu.VMEM),
            pl.BlockSpec(memory_space=pltpu.SMEM),
        ],
        out_shape=[
            jax.ShapeDtypeStruct((parts, stored, pairs, 2 * half), jnp.float32),
            jax.ShapeDtypeStruct((waves,), jnp.int32),
        ],
        scratch_shapes=[pltpu.VMEM((waves, bands), jnp.float32)],
        compiler_params=params(),
        name="sort",
    )(rank, key, wave)


def lane_gather(values, index):
    numbers = lax.GatherDimensionNumbers(
        offset_dims=(),
        collapsed_slice_dims=(1,),
        start_index_map=(1,),
        operand_batching_dims=(0,),
        start_indices_batching_dims=(0,),
    )
    return lax.gather(
        values,
        index[..., None],
        numbers,
        slice_sizes=(1, 1),
        mode=lax.GatherScatterMode.PROMISE_IN_BOUNDS,
    )


def grid_kernel(
    window_ref,
    deep_ref,
    first_ref,
    last_ref,
    code_ref,
    slot_row_ref,
    slot_y_ref,
    potential_ref,
    left_ref,
    right_ref,
    compact_ref,
    out_ref,
    grid_ref,
    windows_ref,
    *,
    size,
    pitch,
    band_pitch,
    wide,
):
    blocks, pairs, lanes = out_ref.shape
    half = lanes // 2
    rows = size * size
    shift = size.bit_length() - 1
    extra = pitch - size
    upper = lax.broadcasted_iota(jnp.int32, (pairs, lanes), 1) // half * half
    parts, _, _, _ = compact_ref.shape
    each = blocks // parts
    inner = lax.broadcasted_iota(jnp.int32, (pairs, lanes), 1) % half
    steps = math.gcd(each, 16)

    def widen(part, carry):
        following = jnp.minimum(part + 1, parts - 1)

        def some(group, carry):
            first = group * steps
            for step in range(steps):
                block = compact_ref[part, first + step]
                if step + 1 < steps:
                    after = compact_ref[part, first + step + 1]
                else:
                    inside = first + steps < each
                    after = compact_ref[
                        jnp.where(inside, part, following), jnp.where(inside, first + steps, 0)
                    ]
                mixed = jnp.where(
                    inner < half // 2,
                    pltpu.roll(block, lanes - half // 2, 1),
                    pltpu.roll(after, half // 2, 1),
                )
                spot = 2 * (part * each + first + step)
                windows_ref[spot] = block
                windows_ref[spot + 1] = mixed
            return carry

        return lax.fori_loop(0, each // steps, some, carry)

    lax.fori_loop(0, parts, widen, 0)

    def expand(group, carry):
        base = group * wide
        place = base + lax.shift_right_logical(base, shift) * extra

        @pl.when(deep_ref[group] == 0)
        def _():
            for step in range(wide):
                row = base + step
                code = jnp.broadcast_to(code_ref[pl.ds(row, 1), :], (pairs, lanes))
                index = (code & (half - 1)) | upper
                value = lane_gather(windows_ref[window_ref[row]], index)
                value = jnp.where(code >= 0, value, 0.0)
                grid_ref[pl.ds(place + step, pairs, stride=band_pitch), :] = value

        @pl.when(deep_ref[group] != 0)
        def _():
            def one(step, carry):
                row = base + step
                code = jnp.broadcast_to(code_ref[pl.ds(row, 1), :], (pairs, lanes))
                index = (code & (half - 1)) | upper
                window = window_ref[row]
                later = jnp.minimum(window + 2, 2 * blocks - 1)
                here = lane_gather(windows_ref[window], index)
                there = lane_gather(windows_ref[later], index)
                value = jnp.where(code < half, here, there)
                value = jnp.where(code >= 0, value, 0.0)
                grid_ref[pl.ds(place + step, pairs, stride=band_pitch), :] = value
                return carry

            lax.fori_loop(0, wide, one, 0)

        return carry

    lax.fori_loop(0, rows // wide, expand, 0)

    left = left_ref[...]
    right = right_ref[...]

    def apply_left(value):
        high, low = split_bf16(value)
        both = dot32(left, jnp.concatenate([high, low], axis=0))
        return both[:size, :] + both[size:, :]

    def apply_right(value):
        high, low = split_bf16(value)
        both = dot32(jnp.concatenate([high, low], axis=1), right)
        return both[:, :lanes] + both[:, lanes:]

    many = math.gcd(size, 16)

    chains = max(1, math.gcd(size // many, 4))
    groups = size // (many * chains)

    def planes(turn, carry):
        base = turn // groups * band_pitch
        offset = turn % groups * (many * chains * pitch)
        for chain in range(chains):
            starts = [
                pl.multiple_of(base + offset + (chain * many + index) * pitch, 8)
                for index in range(many)
            ]
            field = jnp.concatenate([grid_ref[pl.ds(s, size), :] for s in starts], axis=1)
            field = apply_left(field)
            field = jnp.concatenate(
                [field[:, index * lanes : (index + 1) * lanes] for index in range(many)], axis=0
            )
            field = apply_right(field)
            for index, s in enumerate(starts):
                grid_ref[pl.ds(s, size), :] = field[index * size : (index + 1) * size, :]
        return carry

    def columns(turn, carry):
        along = turn % groups * (many * chains)
        base = turn // groups * band_pitch + along
        for chain in range(chains):
            spots = [chain * many + index for index in range(many)]
            field = jnp.concatenate(
                [grid_ref[pl.ds(base + spot, size, stride=pitch), :] for spot in spots], axis=1
            )
            field = apply_left(field)
            weight = jnp.concatenate(
                [
                    potential_ref[pl.ds(pl.multiple_of((along + spot) * size, size), size), :]
                    for spot in spots
                ],
                axis=1,
            )
            field = apply_left(field * weight)
            for index, spot in enumerate(spots):
                grid_ref[pl.ds(base + spot, size, stride=pitch), :] = field[
                    :, index * lanes : (index + 1) * lanes
                ]
        return carry

    turns = pairs * groups
    lax.fori_loop(0, turns, planes, 0)
    lax.fori_loop(0, turns, columns, 0)
    lax.fori_loop(0, turns, planes, 0)

    visits = 12

    def visit(row, wanted, index, value):
        source = row + lax.shift_right_logical(row, shift) * extra
        here = lane_gather(grid_ref[pl.ds(source, pairs, stride=band_pitch), :], index)
        return jnp.where(wanted == row, here, value)

    def slots(block):
        wanted = jnp.broadcast_to(slot_row_ref[pl.ds(block, 1), :], (pairs, lanes))
        index = jnp.broadcast_to(slot_y_ref[pl.ds(block, 1), :], (pairs, lanes))
        return wanted, index

    together = math.gcd(blocks, 16)

    def collect(group, carry):
        longest = 0
        for step in range(together):
            block = group * together + step
            wanted, index = slots(block)
            first = first_ref[block]
            value = jnp.zeros((pairs, lanes), jnp.float32)
            for number in range(visits):
                value = visit(first + number, wanted, index, value)
            out_ref[block] = value
            longest = jnp.maximum(longest, last_ref[block] - first)

        @pl.when(longest >= visits)
        def _():
            for step in range(together):
                block = group * together + step
                wanted, index = slots(block)
                first = first_ref[block]
                out_ref[block] = lax.fori_loop(
                    first + visits,
                    last_ref[block] + 1,
                    lambda row, value: visit(row, wanted, index, value),
                    out_ref[block],
                )

        return carry

    lax.fori_loop(0, blocks // together, collect, 0)


def grid_call(window, deep, first, last, code, slot_row, slot_y, field, left, right, compact, size):
    _, _, pairs, lanes = compact.shape
    blocks = first.shape[0]
    pitch = size + 8
    band_pitch = size * pitch + 8
    smem = pl.BlockSpec(memory_space=pltpu.SMEM)
    vmem = pl.BlockSpec(memory_space=pltpu.VMEM)
    points = 2 * pairs * size**3
    return pl.pallas_call(
        functools.partial(
            grid_kernel,
            size=size,
            pitch=pitch,
            band_pitch=band_pitch,
            wide=size * size // deep.shape[0],
        ),
        in_specs=[smem] * 4 + [vmem] * 7,
        out_specs=vmem,
        out_shape=jax.ShapeDtypeStruct((blocks, pairs, lanes), jnp.float32),
        scratch_shapes=[
            pltpu.VMEM((pairs * band_pitch + 16, lanes), jnp.float32),
            pltpu.VMEM((2 * blocks, pairs, lanes), jnp.float32),
        ],
        compiler_params=params(),
        cost_estimate=pl.CostEstimate(
            flops=36 * size * points, bytes_accessed=4 * points, transcendentals=0
        ),
        name="grid",
    )(window, deep, first, last, code, slot_row, slot_y, field, left, right, compact)


def prepare_kernel(
    known_ref,
    quarter_ref,
    lanes_ref,
    rows_ref,
    code_ref,
    field_ref,
    *,
    skip,
    waves,
    low_count,
    size,
):
    lanes = known_ref.shape[2]
    left_ids, right_ids = rows_ref.shape[0], lanes_ref.shape[0]
    field_rows = code_ref.shape[1] // 2
    wave_rows = waves // lanes
    part = pl.program_id(0)

    def onehot(first, count):
        ids = lax.broadcasted_iota(jnp.int32, (count, lanes), 0).astype(jnp.float32)
        return jnp.concatenate(
            [
                jnp.where(known_ref[0, row : row + 1, :] == ids, 1.0, 0.0).astype(jnp.bfloat16)
                for row in range(first, first + wave_rows)
            ],
            axis=1,
        )

    filled = lax.dot_general(
        onehot(skip, left_ids),
        onehot(skip + wave_rows, right_ids),
        (((1,), (1,)), ((), ())),
        preferred_element_type=jnp.float32,
    )
    sums = dot32(filled.astype(jnp.bfloat16), lanes_ref[...])
    ahead = sums[:, :right_ids]
    counts = jnp.concatenate(
        [sums[:, index * right_ids : (index + 1) * right_ids] for index in (1, 2, 3)], axis=0
    )
    start = dot32(rows_ref[...], counts.astype(jnp.bfloat16)).astype(jnp.int32) + part * waves
    code = ahead.astype(jnp.int32) + (start & (size // 2 - 1))
    code = jnp.where(filled > 0.5, code, -1)
    for low in range(low_count):
        piece = code[:, low * size : (low + 1) * size]
        piece = jnp.concatenate([piece, piece], axis=1)
        for high in range(left_ids // size):
            first = (high * low_count + low) * size
            code_ref[0, first : first + size, :] = piece[high * size : (high + 1) * size, :]
    field = quarter_ref[...].reshape(field_rows, lanes)
    for side in range(2):
        half = field[:, side * size : (side + 1) * size]
        field_ref[0, pl.ds(side, field_rows, stride=2), :] = jnp.concatenate([half, half], axis=1)


def prepare_call(known, quarters, waves, planes_each, size):
    parts, stored, lanes = known.shape
    groups, _, skip, _ = quarters.shape
    low_count = math.gcd(planes_each, 4)
    high_count = planes_each // low_count
    lines = planes_each * size
    eye = np.eye(low_count)
    square = np.ones((size, size))
    before = np.triu(square, 1)
    lanes_table = np.concatenate(
        [
            np.kron(eye, before),
            np.kron(eye, square),
            np.kron(np.triu(np.ones((low_count, low_count)), 1), square),
            np.kron(np.ones((low_count, low_count)), square),
        ],
        axis=1,
    )
    eye = np.eye(high_count)
    rows_table = np.concatenate(
        [
            np.kron(eye, before.T),
            np.kron(eye, square),
            np.kron(np.tril(np.ones((high_count, high_count)), -1), square),
        ],
        axis=1,
    )
    return pl.pallas_call(
        functools.partial(
            prepare_kernel, skip=skip, waves=waves, low_count=low_count, size=size
        ),
        grid=(parts,),
        in_specs=[
            pl.BlockSpec((1, stored, lanes), lambda i: (i, 0, 0)),
            pl.BlockSpec((groups, 1, skip, lanes), lambda i: (0, i, 0, 0)),
            pl.BlockSpec(lanes_table.shape, lambda i: (0, 0)),
            pl.BlockSpec(rows_table.shape, lambda i: (0, 0)),
        ],
        out_specs=[pl.BlockSpec((1, lines, lanes), lambda i: (i, 0, 0))] * 2,
        out_shape=[
            jax.ShapeDtypeStruct((parts, lines, lanes), jnp.int32),
            jax.ShapeDtypeStruct((parts, lines, lanes), jnp.float32),
        ],
        compiler_params=params("arbitrary"),
        cost_estimate=pl.CostEstimate(
            flops=2 * parts * waves * lines * size, bytes_accessed=4 * parts * waves, transcendentals=0
        ),
        name="prepare",
    )(known, quarters, jnp.asarray(lanes_table, jnp.bfloat16), jnp.asarray(rows_table, jnp.bfloat16))


def finish_kernel(rank_ref, where_ref, back_ref, muffin_ref, *refs):
    *all_refs, out_ref, sub_ref, rows_ref = refs
    block, bands = out_ref.shape
    parts, _, _, lanes = back_ref.shape
    half = lanes // 2
    turn = pl.program_id(0)

    @pl.when(turn == 0)
    def _():
        sub_ref[...] = jnp.zeros_like(sub_ref)

        def order(tile, carry):
            start = pl.multiple_of(tile * lanes, lanes)
            pieces = []
            for part in range(parts):
                even = back_ref[part, 2 * tile]
                odd = back_ref[part, 2 * tile + 1]
                pieces.append(jnp.concatenate([even[:, :half], odd[:, :half]], axis=1))
                pieces.append(jnp.concatenate([even[:, half:], odd[:, half:]], axis=1))
            rows_ref[pl.ds(start, lanes), :] = jnp.concatenate(pieces, axis=0).T
            return carry

        lax.fori_loop(0, rows_ref.shape[0] // lanes, order, 0, unroll=4)

    first = turn * block

    def place(index, carry):
        out_ref[pl.ds(index, 1), :] = rows_ref[pl.ds(rank_ref[first + index], 1), :]
        return carry

    lax.fori_loop(0, block, place, 0, unroll=64)
    applied = muffin_ref[...] + out_ref[...].T
    out_ref[...] = applied.T
    high, low = split_bf16(applied)
    both = jnp.concatenate([high, low], axis=0)
    for shift, all_ref in enumerate(all_refs):
        all_high, all_low = split_bf16(all_ref[...])
        main = dot32(both, all_high)
        total = main[:bands, :] + main[bands:, :] + dot32(high, all_low)
        sub_ref[where_ref[shift]] += total

    @pl.when(turn == pl.num_programs(0) - 1)
    def _():
        for group in range(sub_ref.shape[0]):
            sub_ref[group] = sub_ref[group].T * NPW ** (-0.5)


def finish_call(rank, where, back, muffin, columns):
    bands, waves = muffin.shape
    groups = len(columns)
    block = math.gcd(waves, 2048)
    return pl.pallas_call(
        finish_kernel,
        grid=(waves // block,),
        in_specs=[
            pl.BlockSpec(memory_space=pltpu.SMEM),
            pl.BlockSpec(memory_space=pltpu.SMEM),
            pl.BlockSpec(back.shape, lambda i: (0, 0, 0, 0)),
            pl.BlockSpec((bands, block), lambda i: (0, i)),
        ]
        + [pl.BlockSpec((block, bands), lambda i: (i, 0))] * groups,
        out_specs=[
            pl.BlockSpec((block, bands), lambda i: (i, 0)),
            pl.BlockSpec((groups, bands, bands), lambda i: (0, 0, 0)),
        ],
        out_shape=[
            jax.ShapeDtypeStruct((waves, bands), jnp.float32),
            jax.ShapeDtypeStruct((groups, bands, bands), jnp.float32),
        ],
        scratch_shapes=[pltpu.VMEM((waves, bands), jnp.float32)],
        compiler_params=params("arbitrary"),
        name="finish",
    )(rank, where, back, muffin, *columns)


def exchange(array):
    return lax.all_to_all(array, "pw", split_axis=0, concat_axis=0, tiled=True)


def interstitial_tables(size):
    across = np.arange(size)
    angle = 2.0 * np.pi / size * (across[:, None] * across[None, :] % size)
    table = (np.cos(angle) + np.sin(angle)) / math.sqrt(size)
    high = table.astype(jnp.bfloat16).astype(np.float64)
    low = table - high
    zero = np.zeros_like(table)
    left = np.block([[high, high], [low, zero]])
    both = np.eye(2)
    right = np.block(
        [
            [np.kron(both, high), np.kron(both, low)],
            [np.kron(both, high), np.kron(both, zero)],
        ]
    )
    return jnp.asarray(left.astype(jnp.bfloat16)), jnp.asarray(right.astype(jnp.bfloat16))


def whole_step(wave_coeffs, miller, atom_types, positions, sphere_radii, h_blocks, potential):
    pw_count = lax.axis_size("pw")
    pw_index = lax.axis_index("pw")
    local_waves, local_bands = wave_coeffs.shape
    size = potential.shape[1]
    kinds, funcs_each = h_blocks.shape[:2]
    atom_total = atom_types.shape[0]
    miller_float = miller.astype(jnp.float32)
    kinetic = jnp.sum(miller_float * miller_float, axis=0) / 1536.0
    planes_each = size // pw_count
    lines = planes_each * size

    group_count = lax.axis_size("band")
    group = lax.axis_index("band")
    columns = [wave_coeffs]
    for shift in range(1, group_count):
        route = [(index, (index + shift) % group_count) for index in range(group_count)]
        columns.append(lax.ppermute(wave_coeffs, "band", route))
    where = jnp.mod(group - jnp.arange(group_count, dtype=jnp.int32), group_count)

    wrapped = jnp.mod(miller, size)
    line = (wrapped[2] - pw_index * planes_each) * size + wrapped[0]
    key = line * size + wrapped[1]
    rank = jnp.sum((key[:, None] < key[None, :]).astype(jnp.int32), axis=0)
    lanes = 2 * size
    low_count = math.gcd(planes_each, 4)
    plane = wrapped[2] - pw_index * planes_each
    starts = jnp.sum(
        (line[:, None] < jnp.arange(lines, dtype=jnp.int32)[None, :]).astype(jnp.int32), axis=0
    )
    pieces = [
        lax.dynamic_index_in_dim(
            jnp.transpose(potential, (0, 2, 1)).reshape(group_count, -1), group, 0
        ),
        (plane // low_count * size + wrapped[0]).astype(jnp.float32),
        (plane % low_count * size + wrapped[1]).astype(jnp.float32),
        starts.astype(jnp.float32),
    ]
    pieces = [piece.reshape(-1, lanes) for piece in pieces]
    cuts = np.cumsum([piece.shape[0] for piece in pieces])
    pieces.append(jnp.zeros((-int(cuts[-1]) % 8, lanes), jnp.float32))
    known = jnp.concatenate(pieces)
    known = exchange(jnp.broadcast_to(known[None], (pw_count,) + known.shape))
    quarters = lax.all_gather(known[:, : cuts[0]], "band", axis=0, tiled=False)

    send, sorted_key = sort_call(rank, key, wave_coeffs, pw_count, size)
    _, pairs = send.shape[1:3]
    blocks_each = local_waves // size
    keys = sorted_key.astype(jnp.float32).reshape(1, -1, pairs, lanes)
    send = send.at[:, blocks_each:].set(jnp.broadcast_to(keys, (pw_count,) + keys.shape[1:]))
    compact = exchange(send)

    spheres, matching_table, phase = sphere_call(
        atom_types, miller, positions, sphere_radii, wave_coeffs, kinds, funcs_each, 2.0 / size
    )
    onehot = (atom_types[:, None] == jnp.arange(kinds, dtype=jnp.int32)[None, :]).astype(
        jnp.float32
    )
    chosen = jnp.einsum("at,tfk->afk", onehot, h_blocks, precision=PRECISE)

    codes, field = prepare_call(known, quarters, local_waves, planes_each, size)
    codes = codes.reshape(size * size, lanes)
    field = field.reshape(size * size, lanes)
    offsets = jnp.arange(pw_count, dtype=jnp.int32)[:, None]
    all_starts = known[:, cuts[2] : cuts[3]].reshape(pw_count, lines).astype(jnp.int32)
    all_starts = (all_starts + offsets * local_waves).reshape(-1)
    total = pw_count * local_waves
    ends = jnp.concatenate([all_starts[1:], jnp.full((1,), total, jnp.int32)])
    window = jnp.minimum(all_starts // (size // 2), total // (size // 2) - 1)
    reach = (all_starts % (size // 2)) + (ends - all_starts)
    deep = jnp.max(reach.reshape(size, size), axis=1) > size

    all_keys = compact[:, blocks_each:].astype(jnp.int32).reshape(pw_count, -1)
    all_keys = (all_keys + offsets * (lines * size)).reshape(-1, size)
    slot_row = all_keys // size
    slot_y = all_keys % size
    spheres, slot_y = lax.optimization_barrier((spheres, slot_y))
    spheres = lax.psum(spheres, "pw")
    spheres = spheres.reshape(atom_total, funcs_each, local_bands)
    left, right = interstitial_tables(size)
    back = grid_call(
        window,
        deep.astype(jnp.int32),
        slot_row[:, 0],
        slot_row[:, -1],
        codes,
        jnp.concatenate([slot_row, slot_row], axis=1),
        jnp.concatenate([slot_y, slot_y + size], axis=1),
        field,
        left,
        right,
        compact,
        size,
    )
    back = exchange(back.reshape(pw_count, blocks_each, pairs, lanes))
    applied = jnp.einsum("akb,afk->baf", spheres, chosen, precision=PRECISE)
    muffin = muffin_call(
        atom_types, matching_table, phase, applied.reshape(local_bands, -1), kinetic, wave_coeffs
    )
    h_applied, partial = finish_call(rank, where, back, muffin, columns)
    rows_each = group_count * local_bands // pw_count
    gathered = exchange(partial.reshape(pw_count, rows_each, local_bands))
    return (h_applied, jnp.sum(gathered, axis=0))


def solution(mesh):
    in_specs = (P("pw", "band"), P(None, "pw"), P(), P(), P(), P(), P("pw", None, None))
    out_specs = (P("pw", "band"), P("pw", "band"))
    return jax.shard_map(
        whole_step, mesh=mesh, in_specs=in_specs, out_specs=out_specs, check_vma=False
    )
```
